64 devices in a mesh: rep: 4 (over x, y), dp: 16 (over z, core).
Axes of the slice: x: 2, y: 2, z: 8, core: 2. Of those that a mesh axis runs over, the one named last changes fastest.
The devices are a block of a 4x4x8 slice.
Arguments:
- x: bfloat16 [64, 4096, 512], P(('rep', 'dp')), parts along dimension 0
- dy: bfloat16 [64, 4096, 512], P(('rep', 'dp')), parts along dimension 0
- w_gate: bfloat16 [2, 512, 1280], P(None, 'dp')
- w_up: bfloat16 [2, 512, 1280], P(None, 'dp')
- w_down: bfloat16 [2, 1280, 512], P(None, 'dp')
- m_w_gate: float32 [2, 512, 1280], P(None, 'dp')
- m_w_up: float32 [2, 512, 1280], P(None, 'dp')
- m_w_down: float32 [2, 1280, 512], P(None, 'dp')
- v_w_gate: float32 [2, 512, 1280], P(None, 'dp')
- v_w_up: float32 [2, 512, 1280], P(None, 'dp')
- v_w_down: float32 [2, 1280, 512], P(None, 'dp')
Outputs:
- output 1: bfloat16 [8, 512, 1280], P('rep', 'dp'), parts along dimension 0
- output 2: bfloat16 [8, 512, 1280], P('rep', 'dp'), parts along dimension 0
- output 3: bfloat16 [8, 1280, 512], P('rep', 'dp'), parts along dimension 0
- output 4: float32 [8, 512, 1280], P('rep', 'dp'), parts along dimension 0
- output 5: float32 [8, 512, 1280], P('rep', 'dp'), parts along dimension 0
- output 6: float32 [8, 1280, 512], P('rep', 'dp'), parts along dimension 0
- output 7: float32 [8, 512, 1280], P('rep', 'dp'), parts along dimension 0
- output 8: float32 [8, 512, 1280], P('rep', 'dp'), parts along dimension 0
- output 9: float32 [8, 1280, 512], P('rep', 'dp'), parts along dimension 0
There are 4 independent parts. The reference program is written for one: setup_inputs(seed, part) draws one part's arguments, and reference() takes and returns one part's arrays. A program takes and returns all parts, laid end to end along the dimension named above; an argument that names none is the same for every part.
All inputs are finite; a program needn't handle non-finite values.
Results may differ from the reference program's by a relative error of at most 0.0222.
Values are sent between devices in bfloat16 or wider.
A program may use at most 768 MiB of HBM per device.

```python
import jax
import jax.numpy as jnp
from jax import lax

SEQUENCES = 16
TOKENS = 4096
D = 512
FF = 1280
LAYERS = 2
NAMES = ("w_gate", "w_up", "w_down")
SHAPES = {"w_gate": (LAYERS, D, FF), "w_up": (LAYERS, D, FF), "w_down": (LAYERS, FF, D)}


def bump(key, n, height):
    away = (jnp.arange(n, dtype=jnp.int32) - jax.random.randint(key, (), 0, n, jnp.int32)) % n
    return jnp.where(away < n // 8, height, 1.0)


def together(key, own, strength):
    shared = jax.random.normal(key, own.shape[1:], jnp.float32)
    return (own + strength * shared) * lax.rsqrt(1 + strength * strength)


def setup_inputs(seed: int = 0, part: int = 0) -> dict:
    kx, kdy, ka, kb, kz, kf, kh, kl, *keys = jax.random.split(jax.random.key(seed), 8 + 3 * len(NAMES))
    kx, kdy, ka, kb = (jax.random.fold_in(k, part) for k in (kx, kdy, ka, kb))
    kw, km, kv = (keys[i::3] for i in range(3))
    shape = (SEQUENCES, TOKENS, D)
    much_x, much_dy = jax.random.uniform(kz, (2,), jnp.float32, 0.0, 1.0)
    loud = 2.0 ** jax.random.uniform(jax.random.fold_in(kz, 1), (), jnp.float32, -1.0, 2.0)
    layers = 2.0 ** jax.random.uniform(kl, (LAYERS, 1, 1), jnp.float32, -1.0, 1.0)
    x = together(ka, jax.random.normal(kx, shape, jnp.float32), much_x) * bump(kf, D, 4.0)
    dy = together(kb, jax.random.normal(kdy, shape, jnp.float32), much_dy)
    drawn = {"x": x.astype(jnp.bfloat16), "dy": (loud * dy * (SEQUENCES * TOKENS) ** -0.5).astype(jnp.bfloat16)}
    for key, name in zip(kw, NAMES, strict=True):
        w = jax.random.normal(key, SHAPES[name], jnp.float32) * SHAPES[name][1] ** -0.5
        drawn[name] = (w * {"w_gate": 1.0, "w_up": bump(kh, FF, 4.0), "w_down": layers}[name]).astype(jnp.bfloat16)
    for key, name in zip(km, NAMES, strict=True):
        drawn[f"m_{name}"] = 0.1 * jax.random.normal(key, SHAPES[name], jnp.float32)
    for key, name in zip(kv, NAMES, strict=True):
        drawn[f"v_{name}"] = jax.random.uniform(key, SHAPES[name], jnp.float32, 0.005, 0.015)
    return drawn


def matmul(a, w):
    return jnp.dot(a, w, preferred_element_type=jnp.float32).astype(jnp.bfloat16)


def normed(h):
    wide = h.astype(jnp.float32)
    scale = lax.rsqrt(jnp.mean(wide**2, -1, keepdims=True) + 1e-6)
    return (wide * scale).astype(jnp.bfloat16)


def layer(h, w):
    a = normed(h)
    gate = jnp.dot(a, w["w_gate"], preferred_element_type=jnp.float32)
    up = jnp.dot(a, w["w_up"], preferred_element_type=jnp.float32)
    return h + matmul((jax.nn.silu(gate) * up).astype(jnp.bfloat16), w["w_down"])


def adamw(w, m, v, g):
    m = 0.9 * m + 0.1 * g
    v = 0.95 * v + 0.05 * g * g
    step = m * lax.rsqrt(v + 1e-8) + 0.1 * w
    return (w - 0.02 * step).astype(jnp.bfloat16), m, v


def clipped(gradients, sum_of_squares, count):
    factor = jnp.minimum(1.0, 0.5 * lax.rsqrt(sum_of_squares / count + 1e-30))
    return [g * factor for g in gradients]


def stack(weights, h):
    return lax.scan(lambda h, w: (layer(h, w), None), h, weights)[0]


def reference(x, dy, w_gate, w_up, w_down, m_w_gate, m_w_up, m_w_down, v_w_gate, v_w_up, v_w_down):
    weights = dict(zip(NAMES, (w_gate, w_up, w_down), strict=True))

    def take(so_far, sequence):
        h, by_y = sequence
        _, back = jax.vjp(lambda w: stack(w, h), weights)
        return jax.tree.map(lambda total, term: total + term.astype(jnp.float32), so_far, back(by_y)[0]), None

    none_yet = {name: jnp.zeros(w.shape, jnp.float32) for name, w in weights.items()}
    by_weights, _ = lax.scan(take, none_yet, (x, dy))
    gradients = [by_weights[name].astype(jnp.bfloat16).astype(jnp.float32) for name in NAMES]
    gradients = clipped(gradients, sum(jnp.sum(g * g) for g in gradients), sum(g.size for g in gradients))
    new = [
        adamw(w.astype(jnp.float32), m, v, g)
        for w, m, v, g in zip((w_gate, w_up, w_down), (m_w_gate, m_w_up, m_w_down), (v_w_gate, v_w_up, v_w_down), gradients, strict=True)
    ]
    return tuple(one[which] for which in range(3) for one in new)
```

```python
import functools

import jax
import jax.numpy as jnp
from jax import lax
from jax.experimental import pallas as pl
from jax.experimental.pallas import tpu as pltpu
from jax.sharding import PartitionSpec as P

MESH = pl.DeviceIdType.MESH
BF, F32 = jnp.bfloat16, jnp.float32
VMEM_LIMIT = 66_500_000
TILE = 512
WIDE = 1024
COLS = 256


def dot(a, b):
    return jnp.dot(a, b, preferred_element_type=F32)


def dot_t(a, b):
    return lax.dot_general(a, b, (((0,), (0,)), ((), ())), preferred_element_type=F32)


def norm_scale(wide):
    return lax.rsqrt(jnp.mean(wide * wide, -1, keepdims=True) + 1e-6)


def places(n):
    nz = n // 2
    me = lax.axis_index("dp")
    z, core = me // 2, me % 2
    return me, z, core, ((z + 1) % nz) * 2 + core, ((z + nz - 1) % nz) * 2 + core, me + 1 - 2 * core


def barrier(devices):
    sem = pltpu.get_barrier_semaphore()
    for device in devices:
        pl.semaphore_signal(sem, inc=1, device_id={"dp": device}, device_id_type=MESH)
    pl.semaphore_wait(sem, len(devices))


def forward_kernel(n, x_hbm, wg_ref, wu_ref, wd_ref, h1_hbm, hid_hbm, a0_hbm, gu_hbm, d_hbm, dt_hbm,
                   x, a0, hid, gu, d, dt, send_sem, recv_sem, in_sem, out_sem):
    nz = n // 2
    me, z, core, right, left, partner = places(n)
    tokens = x.shape[0]
    steps = tokens // TILE
    load = pltpu.make_async_copy(x_hbm, x, in_sem)
    load.start()
    barrier((right, left, partner))

    more, less = nz // 2, nz - 1 - nz // 2
    parts = [
        (wg_ref.at[0], gu, 0, more, less),
        (wu_ref.at[0], gu, 1, less, more),
        (wd_ref.at[0], d, 0, more, less),
        (wg_ref.at[1], gu, 2, less, more),
        (wu_ref.at[1], gu, 3, more, less),
        (wd_ref.at[1], d, 1, less, more),
    ]
    sent = []

    def block(i, chip, which):
        src, whole, first, _, _ = parts[i]
        rows = src.shape[0]
        at = pl.multiple_of((chip * 2 + which) * rows, 16)
        return whole.at[first, pl.ds(at, rows), :]

    def copy(i, k, src, dst, device):
        return pltpu.make_async_remote_copy(
            src_ref=src, dst_ref=dst, send_sem=send_sem.at[i, k], recv_sem=recv_sem.at[i, k],
            device_id={"dp": device}, device_id_type=MESH,
        )

    def send(i, k, src, dst, device):
        c = copy(i, k, src, dst, device)
        c.start()
        sent.append(c)

    def arrived(i, k, at):
        copy(i, k, at, at, partner).wait_recv()

    def begin(i):
        src = parts[i][0]
        own = block(i, z, core)
        send(i, 0, src, own, right)
        send(i, more, src, own, left)
        send(i, 2 * more, src, own, partner)
        rows = src.shape[0]
        whole, first = parts[i][1], parts[i][2]
        whole[first, pl.ds(pl.multiple_of(me * rows, 16), rows), :] = src[...]

    def relay(i, s):
        _, _, _, hops_right, hops_left = parts[i]
        if s <= hops_right:
            at = block(i, (z + nz - s) % nz, core)
            arrived(i, s - 1, at)
            if s < hops_right:
                send(i, s, at, at, right)
            send(i, 2 * more + s, at, at, partner)
        if s <= hops_left:
            at = block(i, (z + s) % nz, core)
            arrived(i, more + s - 1, at)
            if s < hops_left:
                send(i, more + s, at, at, left)
            send(i, 3 * more + s, at, at, partner)

    def finish(i):
        _, _, _, hops_right, hops_left = parts[i]
        arrived(i, 2 * more, block(i, z, 1 - core))
        for s in range(1, hops_right + 1):
            arrived(i, 2 * more + s, block(i, (z + nz - s) % nz, 1 - core))
        for s in range(1, hops_left + 1):
            arrived(i, 3 * more + s, block(i, (z + s) % nz, 1 - core))

    outs = []

    def store(k, src, dst):
        c = pltpu.make_async_copy(src, dst, out_sem.at[k])
        c.start()
        outs.append(c)

    begin(0)
    begin(1)
    load.wait()

    def norm_step(t, _):
        at = pl.ds(pl.multiple_of(t * TILE, TILE), TILE)
        wide = x[at, :].astype(F32)
        a0[at, :] = (wide * norm_scale(wide)).astype(BF)
        return 0

    relay(0, 1)
    relay(1, 1)
    lax.fori_loop(0, steps // 2, norm_step, 0)
    relay(0, 2)
    relay(1, 2)
    lax.fori_loop(steps // 2, steps, norm_step, 0)
    for s in range(3, more + 1):
        relay(0, s)
        relay(1, s)
    begin(2)
    begin(3)
    finish(0)
    finish(1)
    store(0, a0, a0_hbm)

    def up_step(t, _):
        at = pl.ds(pl.multiple_of(t * TILE, TILE), TILE)
        a = a0[at, :]
        gate = dot(a, gu[0])
        up = dot(a, gu[1])
        hid[at, :] = (gate * jax.nn.sigmoid(gate) * up).astype(BF)
        return 0

    def down_step(t, _):
        at = pl.ds(pl.multiple_of(t * TILE, TILE), TILE)
        x[at, :] = x[at, :] + dot(hid[at, :], d[0]).astype(BF)
        return 0

    quarter = steps // 4
    for q in range(4):
        lax.fori_loop(q * quarter, (q + 1) * quarter, up_step, 0)
        s = q + 1
        if s <= more:
            relay(2, s)
            relay(3, s)
        if s == 3:
            begin(4)
            begin(5)
    for s in range(5, more + 1):
        relay(2, s)
        relay(3, s)
    store(1, hid, hid_hbm)
    relay(4, 1)
    relay(5, 1)
    finish(2)
    dt[...] = d[0].T
    store(2, dt, dt_hbm)
    for q in range(4):
        lax.fori_loop(q * quarter, (q + 1) * quarter, down_step, 0)
        if q == 1:
            relay(4, 2)
            relay(5, 2)
    store(3, x, h1_hbm)
    for s in range(3, more + 1):
        relay(4, s)
        relay(5, s)
    finish(3)
    finish(4)
    finish(5)
    store(4, gu, gu_hbm)
    store(5, d, d_hbm)
    for c in sent:
        c.wait_send()
    for c in outs:
        c.wait()


def forward(n, x, wg, wu, wd):
    tokens, dim = x.shape
    hidden = wg.shape[2]
    anyspace, vmem = pl.BlockSpec(memory_space=pl.ANY), pl.BlockSpec(memory_space=pltpu.VMEM)
    shapes = [(tokens, dim), (tokens, hidden), (tokens, dim), (4, dim, hidden), (2, hidden, dim), (dim, hidden)]
    sems = 4 * (n // 4) + 1
    return pl.pallas_call(
        functools.partial(forward_kernel, n),
        out_shape=[jax.ShapeDtypeStruct(s, BF) for s in shapes],
        in_specs=[anyspace, vmem, vmem, vmem],
        out_specs=[anyspace] * 6,
        scratch_shapes=[
            pltpu.VMEM((tokens, dim), BF),
            pltpu.VMEM((tokens, dim), BF),
            pltpu.VMEM((tokens, hidden), BF),
            pltpu.VMEM((4, dim, hidden), BF),
            pltpu.VMEM((2, hidden, dim), BF),
            pltpu.VMEM((dim, hidden), BF),
            pltpu.SemaphoreType.DMA((6, sems)),
            pltpu.SemaphoreType.DMA((6, sems)),
            pltpu.SemaphoreType.DMA,
            pltpu.SemaphoreType.DMA((6,)),
        ],
        compiler_params=pltpu.CompilerParams(collective_id=0, has_side_effects=True, vmem_limit_bytes=VMEM_LIMIT),
        cost_estimate=pl.CostEstimate(flops=6 * tokens * dim * hidden, bytes_accessed=40 << 20, transcendentals=0),
        name="forward0",
    )(x, wg, wu, wd)


def top_kernel(h1, dy, gu, d, dh, dgu, dd, gt, ut, dt, acc_g, acc_u, acc_d):
    t = pl.program_id(0)

    @pl.when(t == 0)
    def _():
        gt[...] = gu[0].T
        ut[...] = gu[1].T
        dt[...] = d[0].T
        acc_g[...] = jnp.zeros_like(acc_g)
        acc_u[...] = jnp.zeros_like(acc_u)
        acc_d[...] = jnp.zeros_like(acc_d)

    wide = h1[...].astype(F32)
    scale = norm_scale(wide)
    a = (wide * scale).astype(BF)
    by_y = dy[...]
    gate = dot(a, gu[0])
    up = dot(a, gu[1])
    by_hid = dot(by_y, dt[...]).astype(BF).astype(F32)
    sig = jax.nn.sigmoid(gate)
    act = gate * sig
    hid = (act * up).astype(BF)
    by_up = (by_hid * act).astype(BF)
    by_gate = (by_hid * up * (sig + act * (1.0 - sig))).astype(BF)
    acc_d[...] += dot_t(hid, by_y)
    acc_g[...] += dot_t(a, by_gate)
    acc_u[...] += dot_t(a, by_up)
    by_a = (dot(by_gate, gt[...]).astype(BF) + dot(by_up, ut[...]).astype(BF)).astype(F32)
    wide = h1[...].astype(F32)
    by_h = scale * by_a - wide * (scale * scale * scale * jnp.mean(by_a * wide, -1, keepdims=True))
    dh[...] = by_y + by_h.astype(BF)

    @pl.when(t == pl.num_programs(0) - 1)
    def _():
        dgu[0] = acc_g[...].astype(BF)
        dgu[1] = acc_u[...].astype(BF)
        dd[...] = acc_d[...].astype(BF)


def top(h1, dy, gu, d):
    tokens, dim = h1.shape
    hidden = gu.shape[2]
    tile = pl.BlockSpec((TILE, dim), lambda t: (t, 0))
    once = pl.Buffered(1)
    return pl.pallas_call(
        top_kernel,
        grid=(tokens // TILE,),
        out_shape=[
            jax.ShapeDtypeStruct((tokens, dim), BF),
            jax.ShapeDtypeStruct((2, dim, hidden), BF),
            jax.ShapeDtypeStruct((hidden, dim), BF),
        ],
        in_specs=[
            tile,
            tile,
            pl.BlockSpec((2, dim, hidden), lambda t: (1, 0, 0), pipeline_mode=once),
            pl.BlockSpec((1, hidden, dim), lambda t: (1, 0, 0), pipeline_mode=once),
        ],
        out_specs=[
            tile,
            pl.BlockSpec((2, dim, hidden), lambda t: (0, 0, 0), pipeline_mode=once),
            pl.BlockSpec((hidden, dim), lambda t: (0, 0), pipeline_mode=once),
        ],
        scratch_shapes=[
            pltpu.VMEM((hidden, dim), BF),
            pltpu.VMEM((hidden, dim), BF),
            pltpu.VMEM((dim, hidden), BF),
            pltpu.VMEM((dim, hidden), F32),
            pltpu.VMEM((dim, hidden), F32),
            pltpu.VMEM((hidden, dim), F32),
        ],
        compiler_params=pltpu.CompilerParams(vmem_limit_bytes=VMEM_LIMIT),
        cost_estimate=pl.CostEstimate(flops=16 * tokens * dim * hidden, bytes_accessed=24 << 20, transcendentals=0),
        name="layer1",
    )(h1, dy, gu, d)


def backward_kernel(n, a0_hbm, hid_hbm, dh_hbm, gu_hbm, dt_hbm, tgu_hbm, td_hbm, sum_gu, sum_d, squares,
                    a0, hid, dh, gu, dt, tgu1, td1, tgu0, td0, acc_g, acc_u, acc_d,
                    pgu1, pd1, pgu0, pd0, sgu1, sd1, sgu0, sd0, rgu1, rd1, rgu0, rd0, ssq, all_ssq,
                    in_sem, p_send, p_recv, send1, recv1, send0, recv0, q_send, q_recv):
    nz = n // 2
    me, z, core, right, left, partner = places(n)
    tokens, dim = a0.shape
    hidden = dt.shape[1]
    nf = hidden // COLS
    last = nz - 1
    rows_g, rows_d = dim // n, hidden // n

    def load(k, src, dst):
        c = pltpu.make_async_copy(src, dst, in_sem.at[k])
        c.start()
        return c

    first = [load(0, tgu_hbm, tgu1), load(1, td_hbm, td1)]
    half_t = tokens // 2
    second = [load(2, hid_hbm.at[pl.ds(0, half_t), :], hid.at[pl.ds(0, half_t), :]), load(3, dh_hbm, dh)]
    third = [load(4, hid_hbm.at[pl.ds(half_t, half_t), :], hid.at[pl.ds(half_t, half_t), :])]
    fourth = [load(5, a0_hbm, a0), load(6, gu_hbm.at[pl.ds(0, 2)], gu), load(7, dt_hbm, dt)]

    sem = pltpu.get_barrier_semaphore()
    for k in range(1, n):
        pl.semaphore_signal(sem, inc=1, device_id={"dp": (me + k) % n}, device_id_type=MESH)
    pl.semaphore_wait(sem, n - 1)

    def over(k, src, dst):
        return pltpu.make_async_remote_copy(
            src_ref=src, dst_ref=dst, send_sem=p_send.at[k], recv_sem=p_recv.at[k],
            device_id={"dp": partner}, device_id_type=MESH,
        )

    over_gu1 = over(nf, tgu1.at[:, :, 1 - core], pgu1)
    over_d1 = over(nf + 1, td1.at[:, 1 - core], pd1)
    over_d0 = over(nf + 2, td0.at[:, 1 - core], pd0)

    def over_gu0(j):
        return over(j, tgu0.at[j, :, :, 1 - core], pgu0.at[j])

    for c in first:
        c.wait()
    over_gu1.start()
    over_d1.start()
    ssq[...] = jnp.zeros_like(ssq)

    def move(send_ref, recv_ref, send_s, recv_s, device):
        return pltpu.make_async_remote_copy(
            src_ref=send_ref, dst_ref=recv_ref, send_sem=send_s, recv_sem=recv_s, device_id={"dp": device}, device_id_type=MESH
        )

    def squared(v):
        g = v.astype(F32)
        g = g * g
        while g.ndim > 2:
            g = jnp.sum(g, axis=0)
        g = jnp.sum(g, axis=0, keepdims=True)
        total = g[:, 0:128]
        for k in range(1, g.shape[1] // 128):
            total = total + g[:, k * 128 : (k + 1) * 128]
        ssq[0:1, :] += total

    def event(parts, s):
        def chip(way):
            return (z + 2 * nz - 1 - s) % nz if way == 0 else (z + 1 + s) % nz

        def term(part, way, b):
            width = part["width"]
            at = slice(way * width, (way + 1) * width)
            return part["own"](b, at).astype(F32) + part["other"](b, at).astype(F32)

        def wait(part, way):
            part["move"](way, s - 1).wait_recv()

        def go(part, way):
            part["move"](way, s).start()

        @pl.when(s == 0)
        def _():
            for way in range(2):
                for part in parts:
                    part["send"][way, s] = term(part, way, chip(way)).astype(BF)
            for way in range(2):
                for part in parts:
                    go(part, way)

        @pl.when(jnp.logical_and(s > 0, s < last))
        def _():
            for way in range(2):
                for part in parts:
                    wait(part, way)
                    v = part["recv"][way, s - 1].astype(F32) + term(part, way, chip(way))
                    part["send"][way, s] = v.astype(BF)
                for part in parts:
                    go(part, way)

        @pl.when(s == last)
        def _():
            for way in range(2):
                for part in parts:
                    wait(part, way)
                    v = (part["recv"][way, s - 1].astype(F32) + term(part, way, chip(way))).astype(BF)
                    part["put"](way, v)
                    squared(v)

    class Slots:
        def __init__(self, ref, *lead):
            self.ref, self.lead = ref, lead

        def __getitem__(self, k):
            return self.ref[self.lead + k]

        def __setitem__(self, k, v):
            self.ref[self.lead + k] = v

    def part(width, own, other, s_ref, r_ref, sems, k, lead, put):
        def the_move(way, s):
            return move(s_ref.at[lead + (way, s)], r_ref.at[lead + (way, s)], sems[0].at[k, way, s], sems[1].at[k, way, s], right if way == 0 else left)

        return dict(width=width, own=own, other=other, send=Slots(s_ref, *lead), recv=Slots(r_ref, *lead), move=the_move, put=put)

    def put_gu1(way, v):
        w = hidden // 2
        sum_gu[1, :, :, way * w : (way + 1) * w] = v

    def put_d(layer):
        def put(way, v):
            w = dim // 2
            sum_d[layer, :, way * w : (way + 1) * w] = v

        return put

    gu1 = part(hidden // 2, lambda b, at: tgu1[:, b, core, :, at], lambda b, at: pgu1[:, b, :, at], sgu1, rgu1, (send1, recv1), 0, (), put_gu1)
    d1 = part(dim // 2, lambda b, at: td1[b, core, :, at], lambda b, at: pd1[b, :, at], sd1, rd1, (send1, recv1), 1, (), put_d(1))
    d0 = part(dim // 2, lambda b, at: td0[b, core, :, at], lambda b, at: pd0[b, :, at], sd0, rd0, (send1, recv1), 2, (), put_d(0))

    def gu0(j):
        def put(way, v):
            w = COLS // 2
            sum_gu[0, :, :, pl.ds(pl.multiple_of(j * COLS + way * w, w), w)] = v

        return part(COLS // 2, lambda b, at: tgu0[j, :, b, core, :, at], lambda b, at: pgu0[j, :, b, :, at], sgu0, rgu0, (send0, recv0), j, (j,), put)

    for c in second:
        c.wait()
    acc_d[...] = jnp.zeros_like(acc_d)

    def down_step(t, _):
        at = pl.ds(pl.multiple_of(t * TILE, TILE), TILE)
        acc_d[...] += dot_t(hid[at, :], dh[at, :])
        return 0

    steps = tokens // TILE
    lax.fori_loop(0, steps // 2, down_step, 0)
    over_gu1.wait_recv()
    over_d1.wait_recv()
    event((gu1, d1), jnp.int32(0))
    third[0].wait()
    lax.fori_loop(steps // 2, steps, down_step, 0)
    for b in range(nz):
        for c in range(2):
            k = (b * 2 + c) * rows_d
            td0[b, c] = acc_d[k : k + rows_d, :].astype(BF)
    over_d0.start()
    for c in fourth:
        c.wait()

    half = tokens // WIDE // 2

    def wide_step(j):
        cols = pl.ds(pl.multiple_of(j * COLS, COLS), COLS)

        def body(t, _):
            at = pl.ds(pl.multiple_of(t * WIDE, WIDE), WIDE)
            a = a0[at, :]
            gate = dot(a, gu[0, :, cols])
            up = dot(a, gu[1, :, cols])
            by_hid = dot(dh[at, :], dt[:, cols]).astype(BF).astype(F32)
            sig = jax.nn.sigmoid(gate)
            act = gate * sig
            by_up = (by_hid * act).astype(BF)
            by_gate = (by_hid * up * (sig + act * (1.0 - sig))).astype(BF)
            acc_g[...] += dot_t(a, by_gate)
            acc_u[...] += dot_t(a, by_up)
            return 0

        return body

    def events(p, compute):
        @pl.when(p + 1 <= last)
        def _():
            event((gu1, d1), p + 1)

        @pl.when(p == 0)
        def _():
            over_d0.wait_recv()

        @pl.when(p <= last)
        def _():
            event((d0,), p)

        def each(j, _):
            s = p - (2 * j + 2)

            @pl.when(s == 0)
            def _():
                over_gu0(j).wait_recv()

            @pl.when(jnp.logical_and(s >= 0, s <= last))
            def _():
                event((gu0(j),), s)

            return 0

        lax.fori_loop(0, nf, each, 0)

    def phase(p, _):
        j, part_of = p // 2, p % 2

        @pl.when(part_of == 0)
        def _():
            acc_g[...] = jnp.zeros_like(acc_g)
            acc_u[...] = jnp.zeros_like(acc_u)

        lax.fori_loop(part_of * half, part_of * half + half, wide_step(j), 0)

        @pl.when(part_of == 1)
        def _():
            for b in range(nz):
                for c in range(2):
                    k = (b * 2 + c) * rows_g
                    tgu0[j, 0, b, c] = acc_g[k : k + rows_g, :].astype(BF)
                    tgu0[j, 1, b, c] = acc_u[k : k + rows_g, :].astype(BF)
            over_gu0(j).start()

        events(p, True)
        return 0

    def tail(p, _):
        events(p, False)
        return 0

    lax.fori_loop(0, 2 * nf, phase, 0)
    lax.fori_loop(2 * nf, 2 * nf + nz, tail, 0)

    all_ssq[me] = ssq[...]

    def scalar(k):
        return pltpu.make_async_remote_copy(
            src_ref=ssq, dst_ref=all_ssq.at[me], send_sem=q_send.at[k], recv_sem=q_recv.at[k],
            device_id={"dp": (me + k) % n}, device_id_type=MESH,
        )

    def tell(k, _):
        scalar(k).start()
        return 0

    lax.fori_loop(1, n, tell, 0)

    for c in (over_gu1, over_d1, over_d0):
        c.wait_send()

    def left_over(j, _):
        over_gu0(j).wait_send()
        for way in range(2):
            def one(s, _):
                gu0(j)["move"](way, s).wait_send()
                return 0
            lax.fori_loop(0, last, one, 0)
        return 0

    lax.fori_loop(0, nf, left_over, 0)

    def left_one(s, _):
        for way in range(2):
            for q in (gu1, d1, d0):
                q["move"](way, s).wait_send()
        return 0

    lax.fori_loop(0, last, left_one, 0)

    def told(k, _):
        src = (me + n - k) % n
        pltpu.make_async_remote_copy(
            src_ref=ssq, dst_ref=all_ssq.at[src], send_sem=q_send.at[k], recv_sem=q_recv.at[k],
            device_id={"dp": (me + k) % n}, device_id_type=MESH,
        ).wait()
        return 0

    lax.fori_loop(1, n, told, 0)
    squares[...] = jnp.sum(all_ssq[...], axis=0)


def backward(n, a0, hid, dh, gu, dt, tgu, td):
    nz = n // 2
    tokens, dim = a0.shape
    hidden = dt.shape[1]
    nf, last = hidden // COLS, nz - 1
    rg, rd = dim // n, hidden // n
    anyspace, vmem = pl.BlockSpec(memory_space=pl.ANY), pl.BlockSpec(memory_space=pltpu.VMEM)
    V = lambda *s: pltpu.VMEM(s, BF)
    S = lambda *s: pltpu.SemaphoreType.DMA(s)
    slots = [
        V(2, last, 2, rg, hidden // 2),
        V(2, last, rd, dim // 2),
        V(nf, 2, last, 2, rg, COLS // 2),
        V(2, last, rd, dim // 2),
    ]
    return pl.pallas_call(
        functools.partial(backward_kernel, n),
        out_shape=[
            jax.ShapeDtypeStruct((2, 2, rg, hidden), BF),
            jax.ShapeDtypeStruct((2, rd, dim), BF),
            jax.ShapeDtypeStruct((8, 128), F32),
        ],
        in_specs=[anyspace] * 7,
        out_specs=[vmem] * 3,
        scratch_shapes=[
            V(tokens, dim),
            V(tokens, hidden),
            V(tokens, dim),
            V(2, dim, hidden),
            V(dim, hidden),
            V(2, nz, 2, rg, hidden),
            V(nz, 2, rd, dim),
            V(nf, 2, nz, 2, rg, COLS),
            V(nz, 2, rd, dim),
            pltpu.VMEM((dim, COLS), F32),
            pltpu.VMEM((dim, COLS), F32),
            pltpu.VMEM((hidden, dim), F32),
            V(2, nz, rg, hidden),
            V(nz, rd, dim),
            V(nf, 2, nz, rg, COLS),
            V(nz, rd, dim),
            *slots,
            *slots,
            pltpu.VMEM((8, 128), F32),
            pltpu.VMEM((n, 8, 128), F32),
            S(8),
            S(nf + 3),
            S(nf + 3),
            S(3, 2, last),
            S(3, 2, last),
            S(nf, 2, last),
            S(nf, 2, last),
            S(n),
            S(n),
        ],
        compiler_params=pltpu.CompilerParams(collective_id=1, has_side_effects=True, vmem_limit_bytes=VMEM_LIMIT),
        cost_estimate=pl.CostEstimate(flops=12 * tokens * dim * hidden, bytes_accessed=40 << 20, transcendentals=0),
        name="backward0",
    )(a0, hid, dh, gu, dt, tgu.reshape(2, nz, 2, rg, hidden), td.reshape(nz, 2, rd, dim))


def adamw(w, m, v, g):
    m = 0.9 * m + 0.1 * g
    v = 0.95 * v + 0.05 * g * g
    step = m * lax.rsqrt(v + 1e-8) + 0.1 * w
    return (w - 0.02 * step).astype(BF), m, v


def solution(mesh):
    n = mesh.shape["dp"]

    def step(x, dy, *arrays):
        weights, m, v = (arrays[i : i + 3] for i in (0, 3, 6))
        h1, hid, a0, gu, d, dt = forward(n, x[0], *weights)
        dh, tgu, td = top(h1, dy[0], gu, d)
        sum_gu, sum_d, squares = backward(n, a0, hid, dh, gu, dt, tgu, td)
        gradients = [sum_gu[:, 0].astype(F32), sum_gu[:, 1].astype(F32), sum_d.astype(F32)]
        count = n * sum(g.size for g in gradients)
        factor = jnp.minimum(1.0, 0.5 * lax.rsqrt(jnp.sum(squares) / count + 1e-30))
        new = [adamw(w.astype(F32), m, v, g * factor) for w, m, v, g in zip(weights, m, v, gradients, strict=True)]
        return tuple(one[which] for which in range(3) for one in new)

    states, cut = P(("rep", "dp"), None, None), P(None, "dp", None)
    return jax.shard_map(
        step,
        mesh=mesh,
        in_specs=(states, states) + (cut,) * 9,
        out_specs=(P("rep", "dp", None),) * 9,
        check_vma=False,
    )
```

```python
import functools

import jax
import jax.numpy as jnp
from jax import lax
from jax.experimental import pallas as pl
from jax.experimental.pallas import tpu as pltpu
from jax.sharding import PartitionSpec as P

MESH = pl.DeviceIdType.MESH
BF, F32 = jnp.bfloat16, jnp.float32
VMEM_LIMIT = 66_500_000
TILE = 512
WIDE = 1024
COLS = 256


def dot(a, b):
    return jnp.dot(a, b, preferred_element_type=F32)


def dot_t(a, b):
    return lax.dot_general(a, b, (((0,), (0,)), ((), ())), preferred_element_type=F32)


def norm_scale(wide):
    return lax.rsqrt(jnp.mean(wide * wide, -1, keepdims=True) + 1e-6)


def places(n):
    nz = n // 2
    me = lax.axis_index("dp")
    z, core = me // 2, me % 2
    return me, z, core, ((z + 1) % nz) * 2 + core, ((z + nz - 1) % nz) * 2 + core, me + 1 - 2 * core


def barrier(devices):
    sem = pltpu.get_barrier_semaphore()
    for device in devices:
        pl.semaphore_signal(sem, inc=1, device_id={"dp": device}, device_id_type=MESH)
    pl.semaphore_wait(sem, len(devices))


def forward_kernel(n, x_hbm, wg_ref, wu_ref, wd_ref, h1_hbm, hid_hbm, a0_hbm, gu_hbm, dt_hbm,
                   x, a0, hid, gu, d, dt, send_sem, recv_sem, in_sem, out_sem):
    nz = n // 2
    me, z, core, right, left, partner = places(n)
    tokens = x.shape[0]
    steps = tokens // TILE
    load = pltpu.make_async_copy(x_hbm, x, in_sem)
    load.start()
    barrier((right, left, partner))

    more, less = nz // 2, nz - 1 - nz // 2
    parts = [
        (wg_ref.at[0], gu, 0, more, less),
        (wu_ref.at[0], gu, 1, less, more),
        (wd_ref.at[0], d, 0, more, less),
        (wg_ref.at[1], gu, 2, less, more),
        (wu_ref.at[1], gu, 3, more, less),
        (wd_ref.at[1], d, 1, less, more),
    ]
    sent = []

    def block(i, chip, which):
        src, whole, first, _, _ = parts[i]
        rows = src.shape[0]
        at = pl.multiple_of((chip * 2 + which) * rows, 16)
        return whole.at[first, pl.ds(at, rows), :]

    def copy(i, k, src, dst, device):
        return pltpu.make_async_remote_copy(
            src_ref=src, dst_ref=dst, send_sem=send_sem.at[i, k], recv_sem=recv_sem.at[i, k],
            device_id={"dp": device}, device_id_type=MESH,
        )

    def send(i, k, src, dst, device):
        c = copy(i, k, src, dst, device)
        c.start()
        sent.append(c)

    def arrived(i, k, at):
        copy(i, k, at, at, partner).wait_recv()

    def begin(i):
        src = parts[i][0]
        own = block(i, z, core)
        send(i, 0, src, own, right)
        send(i, more, src, own, left)
        send(i, 2 * more, src, own, partner)
        rows = src.shape[0]
        whole, first = parts[i][1], parts[i][2]
        whole[first, pl.ds(pl.multiple_of(me * rows, 16), rows), :] = src[...]

    def relay(i, s):
        _, _, _, hops_right, hops_left = parts[i]
        if s <= hops_right:
            at = block(i, (z + nz - s) % nz, core)
            arrived(i, s - 1, at)
            if s < hops_right:
                send(i, s, at, at, right)
            send(i, 2 * more + s, at, at, partner)
        if s <= hops_left:
            at = block(i, (z + s) % nz, core)
            arrived(i, more + s - 1, at)
            if s < hops_left:
                send(i, more + s, at, at, left)
            send(i, 3 * more + s, at, at, partner)

    def finish(i):
        _, _, _, hops_right, hops_left = parts[i]
        arrived(i, 2 * more, block(i, z, 1 - core))
        for s in range(1, hops_right + 1):
            arrived(i, 2 * more + s, block(i, (z + nz - s) % nz, 1 - core))
        for s in range(1, hops_left + 1):
            arrived(i, 3 * more + s, block(i, (z + s) % nz, 1 - core))

    outs = []

    def store(k, src, dst):
        c = pltpu.make_async_copy(src, dst, out_sem.at[k])
        c.start()
        outs.append(c)

    begin(0)
    begin(1)
    load.wait()

    def norm_step(t, _):
        at = pl.ds(pl.multiple_of(t * TILE, TILE), TILE)
        wide = x[at, :].astype(F32)
        a0[at, :] = (wide * norm_scale(wide)).astype(BF)
        return 0

    relay(0, 1)
    relay(1, 1)
    lax.fori_loop(0, steps // 2, norm_step, 0)
    relay(0, 2)
    relay(1, 2)
    lax.fori_loop(steps // 2, steps, norm_step, 0)
    for s in range(3, more + 1):
        relay(0, s)
        relay(1, s)
    begin(2)
    begin(3)
    finish(0)
    finish(1)
    store(0, a0, a0_hbm)

    def up_step(t, _):
        at = pl.ds(pl.multiple_of(t * TILE, TILE), TILE)
        a = a0[at, :]
        gate = dot(a, gu[0])
        up = dot(a, gu[1])
        hid[at, :] = (gate * jax.nn.sigmoid(gate) * up).astype(BF)
        return 0

    def down_step(t, _):
        at = pl.ds(pl.multiple_of(t * TILE, TILE), TILE)
        x[at, :] = x[at, :] + dot(hid[at, :], d[0]).astype(BF)
        return 0

    moves = [(2, 1), (3, 1), (2, 2), (3, 2), (2, 3), (4, 1), (2, 4), (3, 3), (4, 2), (5, 1), (3, 4), (4, 3), (5, 2), (4, 4), (5, 3), (5, 4)]
    starts = {1: 4, 5: 5}
    each = steps // 8
    for q in range(8):
        lax.fori_loop(q * each, (q + 1) * each, up_step, 0)
        relay(*moves[q])
        if q in starts:
            begin(starts[q])
    store(1, hid, hid_hbm)
    store(2, gu.at[pl.ds(0, 2)], gu_hbm.at[pl.ds(0, 2)])
    finish(2)
    for q in range(8):
        lax.fori_loop(q * each, (q + 1) * each, down_step, 0)
        relay(*moves[8 + q])
        if q == 0:
            dt[0] = d[0].T
            store(3, dt.at[0], dt_hbm.at[0])
    store(4, x, h1_hbm)
    finish(3)
    finish(4)
    store(5, gu.at[pl.ds(2, 2)], gu_hbm.at[pl.ds(2, 2)])
    finish(5)
    dt[1] = d[1].T
    store(6, dt.at[1], dt_hbm.at[1])
    for c in sent:
        c.wait_send()
    for c in outs:
        c.wait()


def forward(n, x, wg, wu, wd):
    tokens, dim = x.shape
    hidden = wg.shape[2]
    anyspace, vmem = pl.BlockSpec(memory_space=pl.ANY), pl.BlockSpec(memory_space=pltpu.VMEM)
    shapes = [(tokens, dim), (tokens, hidden), (tokens, dim), (4, dim, hidden), (2, dim, hidden)]
    sems = 4 * (n // 4) + 1
    return pl.pallas_call(
        functools.partial(forward_kernel, n),
        out_shape=[jax.ShapeDtypeStruct(s, BF) for s in shapes],
        in_specs=[anyspace, vmem, vmem, vmem],
        out_specs=[anyspace] * 5,
        scratch_shapes=[
            pltpu.VMEM((tokens, dim), BF),
            pltpu.VMEM((tokens, dim), BF),
            pltpu.VMEM((tokens, hidden), BF),
            pltpu.VMEM((4, dim, hidden), BF),
            pltpu.VMEM((2, hidden, dim), BF),
            pltpu.VMEM((2, dim, hidden), BF),
            pltpu.SemaphoreType.DMA((6, sems)),
            pltpu.SemaphoreType.DMA((6, sems)),
            pltpu.SemaphoreType.DMA,
            pltpu.SemaphoreType.DMA((7,)),
        ],
        compiler_params=pltpu.CompilerParams(collective_id=0, has_side_effects=True, vmem_limit_bytes=VMEM_LIMIT),
        cost_estimate=pl.CostEstimate(flops=6 * tokens * dim * hidden, bytes_accessed=40 << 20, transcendentals=0),
        name="forward0",
    )(x, wg, wu, wd)


def backward_kernel(n, h1_hbm, dy_hbm, a0_hbm, hid_hbm, gu_hbm, dt_hbm, sum_gu, sum_d, factor,
                    h1, a, dh, acc, gu, gt, dt, hid, tgu, td, pgu, pd, rgu, rd, acc_g, acc_u, acc_d, ssq, all_ssq,
                    in_sem, hid_sem, p_send, p_recv, send_gu, recv_gu, send_d, recv_d, q_send, q_recv):
    nz = n // 2
    me, z, core, right, left, partner = places(n)
    tokens, dim = a.shape
    hidden = dt.shape[1]
    nf = hidden // COLS
    last = nz - 1
    rows_g, rows_d = dim // n, hidden // n
    tiles, slots = tokens // TILE, hid.shape[0]
    half = tokens // WIDE // 2

    def load(k, src, dst):
        return pltpu.make_async_copy(src, dst, in_sem.at[k])

    def load_hid(t):
        slot = t % slots
        return pltpu.make_async_copy(hid_hbm.at[pl.ds(pl.multiple_of(t * TILE, TILE), TILE), :], hid.at[slot], hid_sem.at[slot])

    early = [load(0, h1_hbm, h1), load(1, gu_hbm.at[pl.ds(2, 2)], gu), load(2, dy_hbm, dh), load(3, dt_hbm.at[1], dt)]
    later = [load(4, a0_hbm, a), load(5, gu_hbm.at[pl.ds(0, 2)], gu), load(6, dt_hbm.at[0], dt)]
    for c in early:
        c.start()
    for t in range(slots):
        load_hid(t).start()

    sem = pltpu.get_barrier_semaphore()
    for k in range(1, n):
        pl.semaphore_signal(sem, inc=1, device_id={"dp": (me + k) % n}, device_id_type=MESH)
    pl.semaphore_wait(sem, n - 1)

    ssq[...] = jnp.zeros_like(ssq)
    early[0].wait()

    def begin_step(t, _):
        at = pl.ds(pl.multiple_of(t * TILE, TILE), TILE)
        wide = h1[at, :].astype(F32)
        a[at, :] = (wide * norm_scale(wide)).astype(BF)
        acc[at, :] = jnp.zeros((TILE, dim), F32)
        return 0

    lax.fori_loop(0, tiles, begin_step, 0)
    early[1].wait()
    gt[0] = gu[0].T
    gt[1] = gu[1].T
    early[2].wait()
    early[3].wait()

    def over_gu(q):
        return pltpu.make_async_remote_copy(
            src_ref=tgu.at[q, :, :, 1 - core], dst_ref=pgu.at[q], send_sem=p_send.at[q], recv_sem=p_recv.at[q],
            device_id={"dp": partner}, device_id_type=MESH,
        )

    def over_d(layer):
        k = 2 * nf + layer
        return pltpu.make_async_remote_copy(
            src_ref=td.at[layer, :, 1 - core], dst_ref=pd.at[layer], send_sem=p_send.at[k], recv_sem=p_recv.at[k],
            device_id={"dp": partner}, device_id_type=MESH,
        )

    def chip(way, s):
        return (z + 2 * nz - 1 - s) % nz if way == 0 else (z + 1 + s) % nz

    def squared(v):
        g = v.astype(F32)
        g = g * g
        while g.ndim > 2:
            g = jnp.sum(g, axis=0)
        g = jnp.sum(g, axis=0, keepdims=True)
        total = g[:, 0:128]
        for k in range(1, g.shape[1] // 128):
            total = total + g[:, k * 128 : (k + 1) * 128]
        ssq[0:1, :] += total

    class Gu:
        def __init__(self, q):
            self.q = q

        def cols(self, way):
            return slice(way * (COLS // 2), (way + 1) * (COLS // 2))

        def term(self, way, b):
            return tgu[self.q, :, b, core, :, self.cols(way)].astype(F32) + pgu[self.q, :, b, :, self.cols(way)].astype(F32)

        def keep(self, way, b, v):
            tgu[self.q, :, b, core, :, self.cols(way)] = v

        def got(self, way, s):
            return rgu[self.q, way, s].astype(F32)

        def move(self, way, s):
            return pltpu.make_async_remote_copy(
                src_ref=tgu.at[self.q, :, chip(way, s), core, :, pl.ds(way * (COLS // 2), COLS // 2)], dst_ref=rgu.at[self.q, way, s],
                send_sem=send_gu.at[self.q, way, s], recv_sem=recv_gu.at[self.q, way, s],
                device_id={"dp": right if way == 0 else left}, device_id_type=MESH,
            )

        def put(self, way, v):
            layer, j = 1 - self.q // nf, self.q % nf
            w = COLS // 2
            sum_gu[layer, :, :, pl.ds(pl.multiple_of(j * COLS + way * w, w), w)] = v

    class Down:
        def __init__(self, layer):
            self.layer = layer

        def cols(self, way):
            return slice(way * (dim // 2), (way + 1) * (dim // 2))

        def term(self, way, b):
            return td[self.layer, b, core, :, self.cols(way)].astype(F32) + pd[self.layer, b, :, self.cols(way)].astype(F32)

        def keep(self, way, b, v):
            td[self.layer, b, core, :, self.cols(way)] = v

        def got(self, way, s):
            return rd[self.layer, way, s].astype(F32)

        def move(self, way, s):
            return pltpu.make_async_remote_copy(
                src_ref=td.at[self.layer, chip(way, s), core, :, pl.ds(way * (dim // 2), dim // 2)], dst_ref=rd.at[self.layer, way, s],
                send_sem=send_d.at[self.layer, way, s], recv_sem=recv_d.at[self.layer, way, s],
                device_id={"dp": right if way == 0 else left}, device_id_type=MESH,
            )

        def put(self, way, v):
            sum_d[self.layer, :, self.cols(way)] = v

    def event(part, s):
        @pl.when(s == 0)
        def _():
            for way in range(2):
                part.keep(way, chip(way, s), part.term(way, chip(way, s)).astype(BF))
            for way in range(2):
                part.move(way, s).start()

        @pl.when(jnp.logical_and(s > 0, s < last))
        def _():
            for way in range(2):
                part.move(way, s - 1).wait_recv()
                part.keep(way, chip(way, s), (part.got(way, s - 1) + part.term(way, chip(way, s))).astype(BF))
                part.move(way, s).start()

        @pl.when(s == last)
        def _():
            for way in range(2):
                part.move(way, s - 1).wait_recv()
                v = (part.got(way, s - 1) + part.term(way, chip(way, s))).astype(BF)
                part.put(way, v)
                squared(v)

    first_top, first_down, first_low = 0, 2 * nf, 2 * nf + 2
    end_low = first_low + 2 * nf

    def ready(q):
        return 2 * (q + q // nf)

    def events(p):
        def each_gu(q, _):
            s = p - (ready(q) + 2)

            @pl.when(jnp.logical_and(s >= 0, s <= last))
            def _():
                @pl.when(s == 0)
                def _():
                    over_gu(q).wait_recv()

                event(Gu(q), s)

            return 0

        def each_d(k, _):
            layer = 1 - k
            s = p - (first_down + 2 * k)

            @pl.when(jnp.logical_and(s >= 0, s <= last))
            def _():
                @pl.when(s == 0)
                def _():
                    over_d(layer).wait_recv()

                event(Down(layer), s)

            return 0

        lax.fori_loop(0, 2, each_d, 0)
        lax.fori_loop(0, 2 * nf, each_gu, 0)

    def grads(q):
        for b in range(nz):
            for c in range(2):
                k = (b * 2 + c) * rows_g
                tgu[q, 0, b, c] = acc_g[k : k + rows_g, :].astype(BF)
                tgu[q, 1, b, c] = acc_u[k : k + rows_g, :].astype(BF)
        over_gu(q).start()

    def wide_step(j, with_top):
        cols = pl.ds(pl.multiple_of(j * COLS, COLS), COLS)

        def body(t, _):
            at = pl.ds(pl.multiple_of(t * WIDE, WIDE), WIDE)
            rows = a[at, :]
            by_y = dh[at, :]
            gate = dot(rows, gu[0, :, cols])
            up = dot(rows, gu[1, :, cols])
            by_hid = dot(by_y, dt[:, cols]).astype(BF).astype(F32)
            sig = jax.nn.sigmoid(gate)
            act = gate * sig
            by_up = (by_hid * act).astype(BF)
            by_gate = (by_hid * up * (sig + act * (1.0 - sig))).astype(BF)
            acc_g[...] += dot_t(rows, by_gate)
            acc_u[...] += dot_t(rows, by_up)
            if with_top:
                acc_d[...] += dot_t(by_y, (act * up).astype(BF))
                acc[at, :] += dot(by_gate, gt[0, cols, :]) + dot(by_up, gt[1, cols, :])
            return 0

        return body

    def top_end(t, _):
        at = pl.ds(pl.multiple_of(t * TILE, TILE), TILE)
        wide = h1[at, :].astype(F32)
        scale = norm_scale(wide)
        by_a = acc[at, :].astype(BF).astype(F32)
        by_h = scale * by_a - wide * (scale * scale * scale * jnp.mean(by_a * wide, -1, keepdims=True))
        dh[at, :] = dh[at, :] + by_h.astype(BF)
        return 0

    def down_step(t, _):
        load_hid(t).wait()
        acc[0:hidden, :] += dot_t(hid[t % slots], dh[pl.ds(pl.multiple_of(t * TILE, TILE), TILE), :])

        @pl.when(t + slots < tiles)
        def _():
            load_hid(t + slots).start()

        return 0

    def zero():
        acc_g[...] = jnp.zeros_like(acc_g)
        acc_u[...] = jnp.zeros_like(acc_u)

    def phase(p, _):
        part_of = p % 2
        lo = part_of * half

        @pl.when(p < first_down)
        def _():
            j = p // 2

            @pl.when(part_of == 0)
            def _():
                zero()
                acc_d[...] = jnp.zeros_like(acc_d)

            lax.fori_loop(lo, lo + half, wide_step(j, True), 0)

            @pl.when(part_of == 1)
            def _():
                grads(j)
                down = acc_d[...].T.astype(BF)
                for i in range(COLS // 16):
                    row = j * COLS + i * 16
                    device = row // rows_d
                    td[1, device // 2, device % 2, pl.ds(pl.multiple_of(row % rows_d, 16), 16), :] = down[i * 16 : i * 16 + 16, :]

            @pl.when(p == first_down - 1)
            def _():
                over_d(1).start()
                for c in later:
                    c.start()
                lax.fori_loop(0, tiles, top_end, 0)

        @pl.when(jnp.logical_and(p >= first_down, p < first_low))
        def _():
            @pl.when(part_of == 0)
            def _():
                acc[0:hidden, :] = jnp.zeros((hidden, dim), F32)

            lax.fori_loop(part_of * (tiles // 2), part_of * (tiles // 2) + tiles // 2, down_step, 0)

            @pl.when(part_of == 1)
            def _():
                for b in range(nz):
                    for c in range(2):
                        k = (b * 2 + c) * rows_d
                        td[0, b, c] = acc[k : k + rows_d, :].astype(BF)
                over_d(0).start()
                for c in later:
                    c.wait()

        @pl.when(jnp.logical_and(p >= first_low, p < end_low))
        def _():
            j = (p - first_low) // 2

            @pl.when(part_of == 0)
            def _():
                zero()

            lax.fori_loop(lo, lo + half, wide_step(j, False), 0)

            @pl.when(part_of == 1)
            def _():
                grads(nf + j)

        events(p)
        return 0

    lax.fori_loop(0, end_low + nz, phase, 0)

    all_ssq[me] = ssq[...]

    def scalar(k, slot):
        return pltpu.make_async_remote_copy(
            src_ref=ssq, dst_ref=all_ssq.at[slot], send_sem=q_send.at[k], recv_sem=q_recv.at[k],
            device_id={"dp": (me + k) % n}, device_id_type=MESH,
        )

    def tell(k, _):
        scalar(k, me).start()
        return 0

    lax.fori_loop(1, n, tell, 0)

    def left_gu(q, _):
        over_gu(q).wait_send()

        def one(s, _):
            for way in range(2):
                Gu(q).move(way, s).wait_send()
            return 0

        lax.fori_loop(0, last, one, 0)
        return 0

    def left_d(layer, _):
        over_d(layer).wait_send()

        def one(s, _):
            for way in range(2):
                Down(layer).move(way, s).wait_send()
            return 0

        lax.fori_loop(0, last, one, 0)
        return 0

    lax.fori_loop(0, 2 * nf, left_gu, 0)
    lax.fori_loop(0, 2, left_d, 0)

    def told(k, _):
        scalar(k, (me + n - k) % n).wait()
        return 0

    lax.fori_loop(1, n, told, 0)
    total = jnp.sum(jnp.sum(jnp.sum(all_ssq[...], axis=0), axis=0, keepdims=True), axis=1, keepdims=True)
    count = 3 * 2 * dim * hidden
    factor[...] = jnp.broadcast_to(jnp.minimum(1.0, 0.5 * lax.rsqrt(total / count + 1e-30)), factor.shape)


def backward(n, h1, dy, a0, hid, gu, dt):
    nz = n // 2
    tokens, dim = a0.shape
    hidden = dt.shape[2]
    nf, last = hidden // COLS, nz - 1
    rg, rd = dim // n, hidden // n
    anyspace, vmem = pl.BlockSpec(memory_space=pl.ANY), pl.BlockSpec(memory_space=pltpu.VMEM)
    V = lambda *s: pltpu.VMEM(s, BF)
    W = lambda *s: pltpu.VMEM(s, F32)
    S = lambda *s: pltpu.SemaphoreType.DMA(s)
    return pl.pallas_call(
        functools.partial(backward_kernel, n),
        out_shape=[
            jax.ShapeDtypeStruct((2, 2, rg, hidden), BF),
            jax.ShapeDtypeStruct((2, rd, dim), BF),
            jax.ShapeDtypeStruct((8, 128), F32),
        ],
        in_specs=[anyspace] * 6,
        out_specs=[vmem] * 3,
        scratch_shapes=[
            V(tokens, dim),
            V(tokens, dim),
            V(tokens, dim),
            W(tokens, dim),
            V(2, dim, hidden),
            V(2, hidden, dim),
            V(dim, hidden),
            V(3, TILE, hidden),
            V(2 * nf, 2, nz, 2, rg, COLS),
            V(2, nz, 2, rd, dim),
            V(2 * nf, 2, nz, rg, COLS),
            V(2, nz, rd, dim),
            V(2 * nf, 2, last, 2, rg, COLS // 2),
            V(2, 2, last, rd, dim // 2),
            W(dim, COLS),
            W(dim, COLS),
            W(dim, COLS),
            W(8, 128),
            W(n, 8, 128),
            S(7),
            S(3),
            S(2 * nf + 2),
            S(2 * nf + 2),
            S(2 * nf, 2, last),
            S(2 * nf, 2, last),
            S(2, 2, last),
            S(2, 2, last),
            S(n),
            S(n),
        ],
        compiler_params=pltpu.CompilerParams(collective_id=1, has_side_effects=True, vmem_limit_bytes=VMEM_LIMIT),
        cost_estimate=pl.CostEstimate(flops=28 * tokens * dim * hidden, bytes_accessed=40 << 20, transcendentals=0),
        name="backward",
    )(h1, dy, a0, hid, gu, dt)


def adamw(w, m, v, g):
    m = 0.9 * m + 0.1 * g
    v = 0.95 * v + 0.05 * g * g
    step = m * lax.rsqrt(v + 1e-8) + 0.1 * w
    return (w - 0.02 * step).astype(BF), m, v


def solution(mesh):
    n = mesh.shape["dp"]

    def step(x, dy, *arrays):
        weights, m, v = (arrays[i : i + 3] for i in (0, 3, 6))
        h1, hid, a0, gu, dt = forward(n, x[0], *weights)
        sum_gu, sum_d, factor = backward(n, h1, dy[0], a0, hid, gu, dt)
        gradients = [sum_gu[:, 0].astype(F32), sum_gu[:, 1].astype(F32), sum_d.astype(F32)]
        factor = factor[0, 0]
        new = [adamw(w.astype(F32), m, v, g * factor) for w, m, v, g in zip(weights, m, v, gradients, strict=True)]
        return tuple(one[which] for which in range(3) for one in new)

    states, cut = P(("rep", "dp"), None, None), P(None, "dp", None)
    return jax.shard_map(
        step,
        mesh=mesh,
        in_specs=(states, states) + (cut,) * 9,
        out_specs=(P("rep", "dp", None),) * 9,
        check_vma=False,
    )
```

```python
import functools

import jax
import jax.numpy as jnp
from jax import lax
from jax.experimental import pallas as pl
from jax.experimental.pallas import tpu as pltpu
from jax.sharding import PartitionSpec as P

MESH = pl.DeviceIdType.MESH
BF, F32 = jnp.bfloat16, jnp.float32
VMEM_LIMIT = 66_500_000
TILE = 512
WIDE = 1024
COLS = 256
DIRECT = 3
WAIT = 4


def dot(a, b):
    return jnp.dot(a, b, preferred_element_type=F32)


def dot_t(a, b):
    return lax.dot_general(a, b, (((0,), (0,)), ((), ())), preferred_element_type=F32)


def norm_scale(wide):
    return lax.rsqrt(jnp.mean(wide * wide, -1, keepdims=True) + 1e-6)


def places(n):
    nz = n // 2
    me = lax.axis_index("dp")
    z, core = me // 2, me % 2
    return me, z, core, ((z + 1) % nz) * 2 + core, ((z + nz - 1) % nz) * 2 + core, me + 1 - 2 * core


def barrier(devices):
    sem = pltpu.get_barrier_semaphore()
    for device in devices:
        pl.semaphore_signal(sem, inc=1, device_id={"dp": device}, device_id_type=MESH)
    pl.semaphore_wait(sem, len(devices))


def forward_kernel(n, x_hbm, wg_ref, wu_ref, wd_ref, h1_hbm, a1_hbm, hid_hbm, a0_hbm, gu_hbm, dt_hbm,
                   x, a0, hid, gu, d, dt, send_sem, recv_sem, in_sem, out_sem):
    nz = n // 2
    me, z, core, right, left, partner = places(n)
    tokens = x.shape[0]
    steps = tokens // TILE
    load = pltpu.make_async_copy(x_hbm, x, in_sem)
    load.start()
    barrier((right, left, partner))

    more, less = nz // 2, nz - 1 - nz // 2
    g_rows, d_rows = wg_ref.shape[1], wd_ref.shape[1]
    g_half = g_rows // 2
    parts = []
    for lo in (0, g_half):
        parts.append((wg_ref.at[0, pl.ds(lo, g_half)], g_rows, lo, gu, 0, more, less))
        parts.append((wu_ref.at[0, pl.ds(lo, g_half)], g_rows, lo, gu, 1, less, more))
    parts += [
        (wd_ref.at[0], d_rows, 0, d, 0, more, less),
        (wg_ref.at[1], g_rows, 0, gu, 2, less, more),
        (wu_ref.at[1], g_rows, 0, gu, 3, more, less),
        (wd_ref.at[1], d_rows, 0, d, 1, less, more),
    ]
    sent = []

    def block(i, chip, which):
        src, rows, lo, whole, first, _, _ = parts[i]
        at = pl.multiple_of((chip * 2 + which) * rows + lo, 16)
        return whole.at[first, pl.ds(at, src.shape[0]), :]

    def copy(i, k, src, dst, device):
        return pltpu.make_async_remote_copy(
            src_ref=src, dst_ref=dst, send_sem=send_sem.at[i, k], recv_sem=recv_sem.at[i, k],
            device_id={"dp": device}, device_id_type=MESH,
        )

    def send(i, k, src, dst, device):
        c = copy(i, k, src, dst, device)
        c.start()
        sent.append(c)

    def arrived(i, k, at):
        copy(i, k, at, at, partner).wait_recv()

    def begin(i):
        src, rows, lo, whole, first, _, _ = parts[i]
        own = block(i, z, core)
        send(i, 0, src, own, right)
        send(i, more, src, own, left)
        send(i, 2 * more, src, own, partner)
        whole[first, pl.ds(pl.multiple_of(me * rows + lo, 16), src.shape[0]), :] = src[...]

    def relay(i, s):
        hops_right, hops_left = parts[i][5:]
        if s <= hops_right:
            at = block(i, (z + nz - s) % nz, core)
            arrived(i, s - 1, at)
            if s < hops_right:
                send(i, s, at, at, right)
            send(i, 2 * more + s, at, at, partner)
        if s <= hops_left:
            at = block(i, (z + s) % nz, core)
            arrived(i, more + s - 1, at)
            if s < hops_left:
                send(i, more + s, at, at, left)
            send(i, 3 * more + s, at, at, partner)

    def finish(i):
        hops_right, hops_left = parts[i][5:]
        arrived(i, 2 * more, block(i, z, 1 - core))
        for s in range(1, hops_right + 1):
            arrived(i, 2 * more + s, block(i, (z + nz - s) % nz, 1 - core))
        for s in range(1, hops_left + 1):
            arrived(i, 3 * more + s, block(i, (z + s) % nz, 1 - core))

    outs = []

    def store(k, src, dst):
        c = pltpu.make_async_copy(src, dst, out_sem.at[k])
        c.start()
        outs.append(c)

    for i in range(4):
        begin(i)
    load.wait()

    def norm_step(t, _):
        at = pl.ds(pl.multiple_of(t * TILE, TILE), TILE)
        wide = x[at, :].astype(F32)
        a0[at, :] = (wide * norm_scale(wide)).astype(BF)
        return 0

    for s in range(1, more):
        if s < 3:
            lax.fori_loop((s - 1) * (steps // 2), s * (steps // 2), norm_step, 0)
        for i in range(4):
            relay(i, s)
    for i in range(4, 7):
        begin(i)
    for i in range(4):
        relay(i, more)
    for i in range(4):
        finish(i)
    store(0, a0, a0_hbm)

    def up_step(t, _):
        at = pl.ds(pl.multiple_of(t * TILE, TILE), TILE)
        a = a0[at, :]
        gate = dot(a, gu[0])
        up = dot(a, gu[1])
        hid[at, :] = (gate * jax.nn.sigmoid(gate) * up).astype(BF)
        return 0

    def down_step(t, _):
        at = pl.ds(pl.multiple_of(t * TILE, TILE), TILE)
        h = x[at, :] + dot(hid[at, :], d[0]).astype(BF)
        x[at, :] = h
        wide = h.astype(F32)
        a0[at, :] = (wide * norm_scale(wide)).astype(BF)
        return 0

    moves = [
        [(4, 1)], [(5, 1)], [(4, 2), (6, 1)], [(5, 2)], [(4, 3)], [(6, 2)], [(4, 4)], [(5, 3), (7, 1)],
        [(6, 3)], [], [(5, 4)], [(7, 2)], [], [(6, 4)], [(7, 3)], [(7, 4)],
    ]
    each = steps // 8
    for q in range(8):
        lax.fori_loop(q * each, (q + 1) * each, up_step, 0)
        for k in moves[q]:
            relay(*k)
        if q == 3:
            begin(7)
    store(1, hid, hid_hbm)
    store(2, gu.at[pl.ds(0, 2)], gu_hbm.at[pl.ds(0, 2)])
    outs[0].wait()
    finish(4)
    for q in range(8):
        lax.fori_loop(q * each, (q + 1) * each, down_step, 0)
        for k in moves[8 + q]:
            relay(*k)
        if q == 0:
            dt[0] = d[0].T
            store(3, dt.at[0], dt_hbm.at[0])
    store(4, x, h1_hbm)
    store(7, a0, a1_hbm)
    finish(5)
    finish(6)
    store(5, gu.at[pl.ds(2, 2)], gu_hbm.at[pl.ds(2, 2)])
    finish(7)
    dt[1] = d[1].T
    store(6, dt.at[1], dt_hbm.at[1])
    for c in sent:
        c.wait_send()
    for c in outs[1:]:
        c.wait()


def forward(n, x, wg, wu, wd):
    tokens, dim = x.shape
    hidden = wg.shape[2]
    anyspace, vmem = pl.BlockSpec(memory_space=pl.ANY), pl.BlockSpec(memory_space=pltpu.VMEM)
    shapes = [(tokens, dim), (tokens, dim), (tokens, hidden), (tokens, dim), (4, dim, hidden), (2, dim, hidden)]
    sems = 4 * (n // 4) + 1
    return pl.pallas_call(
        functools.partial(forward_kernel, n),
        out_shape=[jax.ShapeDtypeStruct(s, BF) for s in shapes],
        in_specs=[anyspace, vmem, vmem, vmem],
        out_specs=[anyspace] * 6,
        scratch_shapes=[
            pltpu.VMEM((tokens, dim), BF),
            pltpu.VMEM((tokens, dim), BF),
            pltpu.VMEM((tokens, hidden), BF),
            pltpu.VMEM((4, dim, hidden), BF),
            pltpu.VMEM((2, hidden, dim), BF),
            pltpu.VMEM((2, dim, hidden), BF),
            pltpu.SemaphoreType.DMA((8, sems)),
            pltpu.SemaphoreType.DMA((8, sems)),
            pltpu.SemaphoreType.DMA,
            pltpu.SemaphoreType.DMA((8,)),
        ],
        compiler_params=pltpu.CompilerParams(collective_id=0, has_side_effects=True, vmem_limit_bytes=VMEM_LIMIT),
        cost_estimate=pl.CostEstimate(flops=6 * tokens * dim * hidden, bytes_accessed=40 << 20, transcendentals=0),
        name="forward0",
    )(x, wg, wu, wd)


def backward_kernel(n, h1_hbm, a1_hbm, dy_hbm, a0_hbm, hid_hbm, gu_hbm, dt_hbm, sum_gu, sum_d, factor,
                    h1, a, dh, acc, gu, gt, dt, hid, tgu, td, pgu, pd, rgu, rd, rs, acc_gu, acc_d, ssq, all_ssq,
                    in_sem, hid_sem, p_send, p_recv, send_gu, recv_gu, send_d, recv_d, send_s, recv_s, q_send, q_recv):
    nz = n // 2
    me, z, core, right, left, partner = places(n)
    tokens, dim = a.shape
    hidden = dt.shape[1]
    nf = hidden // COLS
    last = nz - 1
    rows_g, rows_d = dim // n, hidden // n
    tiles, slots = tokens // TILE, hid.shape[0]
    half = tokens // WIDE // 2

    def load(k, src, dst):
        return pltpu.make_async_copy(src, dst, in_sem.at[k])

    def load_hid(t):
        slot = t % slots
        return pltpu.make_async_copy(hid_hbm.at[pl.ds(pl.multiple_of(t * TILE, TILE), TILE), :], hid.at[slot], hid_sem.at[slot])

    early = [load(1, gu_hbm.at[pl.ds(2, 2)], gu), load(7, a1_hbm, a), load(2, dy_hbm, dh), load(3, dt_hbm.at[1], dt), load(0, h1_hbm, h1)]
    later = [load(4, a0_hbm, a), load(5, gu_hbm.at[pl.ds(0, 2)], gu), load(6, dt_hbm.at[0], dt)]
    for c in early:
        c.start()
    for t in range(slots):
        load_hid(t).start()

    sem = pltpu.get_barrier_semaphore()
    for k in range(1, n):
        pl.semaphore_signal(sem, inc=1, device_id={"dp": (me + k) % n}, device_id_type=MESH)
    pl.semaphore_wait(sem, n - 1)

    ssq[...] = jnp.zeros_like(ssq)

    def begin_step(t, _):
        acc[pl.ds(pl.multiple_of(t * TILE, TILE), TILE), :] = jnp.zeros((TILE, dim), F32)
        return 0

    lax.fori_loop(0, tiles, begin_step, 0)
    early[0].wait()
    for j in range(nf):
        for i in range(2):
            gt[j, i * COLS : (i + 1) * COLS, :] = gu[i, :, j * COLS : (j + 1) * COLS].T
    for c in early[1:4]:
        c.wait()

    def over_gu(q):
        return pltpu.make_async_remote_copy(
            src_ref=tgu.at[q, :, :, 1 - core], dst_ref=pgu.at[q], send_sem=p_send.at[q], recv_sem=p_recv.at[q],
            device_id={"dp": partner}, device_id_type=MESH,
        )

    def over_d(layer):
        k = 2 * nf + layer
        return pltpu.make_async_remote_copy(
            src_ref=td.at[layer, :, 1 - core], dst_ref=pd.at[layer], send_sem=p_send.at[k], recv_sem=p_recv.at[k],
            device_id={"dp": partner}, device_id_type=MESH,
        )

    def chip(way, s):
        return (z + 2 * nz - 1 - s) % nz if way == 0 else (z + 1 + s) % nz

    def squared(v):
        g = v.astype(F32)
        g = g * g
        while g.ndim > 2:
            g = jnp.sum(g, axis=0)
        g = jnp.sum(g, axis=0, keepdims=True)
        total = g[:, 0:128]
        for k in range(1, g.shape[1] // 128):
            total = total + g[:, k * 128 : (k + 1) * 128]
        ssq[0:1, :] += total

    class Gu:
        def __init__(self, q):
            self.q = q

        def over(self):
            return over_gu(self.q)

        def cols(self, way):
            return slice(way * (COLS // 2), (way + 1) * (COLS // 2))

        def term(self, way, b):
            return tgu[self.q, :, b, core, :, self.cols(way)].astype(F32) + pgu[self.q, :, b, :, self.cols(way)].astype(F32)

        def keep(self, way, b, v):
            tgu[self.q, :, b, core, :, self.cols(way)] = v

        def got(self, way, s):
            return rgu[self.q, way, s].astype(F32)

        def move(self, way, s):
            return pltpu.make_async_remote_copy(
                src_ref=tgu.at[self.q, :, chip(way, s), core, :, pl.ds(way * (COLS // 2), COLS // 2)], dst_ref=rgu.at[self.q, way, s],
                send_sem=send_gu.at[self.q, way, s], recv_sem=recv_gu.at[self.q, way, s],
                device_id={"dp": right if way == 0 else left}, device_id_type=MESH,
            )

        def put(self, way, v):
            layer, j = 1 - self.q // nf, self.q % nf
            w = COLS // 2
            sum_gu[layer, :, :, pl.ds(pl.multiple_of(j * COLS + way * w, w), w)] = v

    class Down:
        def __init__(self, layer):
            self.layer = layer

        def over(self):
            return over_d(self.layer)

        def cols(self, way):
            return slice(way * (dim // 2), (way + 1) * (dim // 2))

        def term(self, way, b):
            return td[self.layer, b, core, :, self.cols(way)].astype(F32) + pd[self.layer, b, :, self.cols(way)].astype(F32)

        def keep(self, way, b, v):
            td[self.layer, b, core, :, self.cols(way)] = v

        def got(self, way, s):
            return rd[self.layer, way, s].astype(F32)

        def move(self, way, s):
            return pltpu.make_async_remote_copy(
                src_ref=td.at[self.layer, chip(way, s), core, :, pl.ds(way * (dim // 2), dim // 2)], dst_ref=rd.at[self.layer, way, s],
                send_sem=send_d.at[self.layer, way, s], recv_sem=recv_d.at[self.layer, way, s],
                device_id={"dp": right if way == 0 else left}, device_id_type=MESH,
            )

        def put(self, way, v):
            sum_d[self.layer, :, self.cols(way)] = v

    def event(part, s):
        @pl.when(s == 0)
        def _():
            part.over().wait()
            for way in range(2):
                part.keep(way, chip(way, s), part.term(way, chip(way, s)).astype(BF))
            for way in range(2):
                part.move(way, s).start()

        @pl.when(jnp.logical_and(s > 0, s < last))
        def _():
            for way in range(2):
                part.move(way, s - 1).wait()
                part.keep(way, chip(way, s), (part.got(way, s - 1) + part.term(way, chip(way, s))).astype(BF))
                part.move(way, s).start()

        @pl.when(s == last)
        def _():
            for way in range(2):
                part.move(way, s - 1).wait()
                v = (part.got(way, s - 1) + part.term(way, chip(way, s))).astype(BF)
                part.put(way, v)
                squared(v)

    first_top, first_down, first_low = 0, 2 * nf, 2 * nf + 2
    end_low = first_low + 2 * nf

    def ready(q):
        return 2 * (q + q // nf)

    rings = 2 * nf - DIRECT
    order = sorted(range(1, nz), key=lambda k: -min(k, nz - k))

    def straight(i, k):
        to = (z + k) % nz
        return pltpu.make_async_remote_copy(
            src_ref=tgu.at[rings + i, :, to, core], dst_ref=rs.at[i, k], send_sem=send_s.at[i, k], recv_sem=recv_s.at[i, k],
            device_id={"dp": to * 2 + core}, device_id_type=MESH,
        )

    def both_terms(q, b):
        return tgu[q, :, b, core].astype(F32) + pgu[q, :, b].astype(F32)

    def events(p):
        def each_direct(i, _):
            q = rings + i
            s = p - (ready(q) + 2)

            @pl.when(s == 0)
            def _():
                over_gu(q).wait()
                for k in order:
                    to = (z + k) % nz
                    tgu[q, :, to, core] = both_terms(q, to).astype(BF)
                    straight(i, k).start()

            @pl.when(s == WAIT)
            def _():
                v = both_terms(q, z)
                for k in range(1, nz):
                    straight(i, k).wait()
                    v = v + rs[i, k].astype(F32)
                v = v.astype(BF)
                sum_gu[0, :, :, pl.ds(pl.multiple_of((q - nf) * COLS, COLS), COLS)] = v
                squared(v)

            return 0

        def each_gu(q, _):
            s = p - (ready(q) + 2)

            @pl.when(jnp.logical_and(s >= 0, s <= last))
            def _():
                event(Gu(q), s)

            return 0

        def each_d(k, _):
            s = p - (first_down + 2 * k)

            @pl.when(jnp.logical_and(s >= 0, s <= last))
            def _():
                event(Down(1 - k), s)

            return 0

        @pl.when(p >= ready(rings) + 2)
        def _():
            lax.fori_loop(0, DIRECT, each_direct, 0)

        @pl.when(p >= first_down)
        def _():
            lax.fori_loop(0, 2, each_d, 0)

        lax.fori_loop(0, rings, each_gu, 0)

    def grads(q):
        for b in range(nz):
            for c in range(2):
                k = (b * 2 + c) * rows_g
                for i in range(2):
                    tgu[q, i, b, c] = acc_gu[k : k + rows_g, i * COLS : (i + 1) * COLS].astype(BF)
        over_gu(q).start()

    def wide_step(j, with_top):
        cols = pl.ds(pl.multiple_of(j * COLS, COLS), COLS)

        def body(t, _):
            at = pl.ds(pl.multiple_of(t * WIDE, WIDE), WIDE)
            rows = a[at, :]
            by_y = dh[at, :]
            gate = dot(rows, gu[0, :, cols])
            up = dot(rows, gu[1, :, cols])
            by_hid = dot(by_y, dt[:, cols]).astype(BF).astype(F32)
            sig = jax.nn.sigmoid(gate)
            act = gate * sig
            by_up = (by_hid * act).astype(BF)
            by_gate = (by_hid * up * (sig + act * (1.0 - sig))).astype(BF)
            by_both = jnp.concatenate([by_gate, by_up], axis=1)
            acc_gu[...] += dot_t(rows, by_both)
            if with_top:
                acc_d[...] += dot_t(by_y, (act * up).astype(BF))
                acc[at, :] += dot(by_both, gt[j])
            return 0

        return body

    def top_end(t, _):
        at = pl.ds(pl.multiple_of(t * TILE, TILE), TILE)
        wide = h1[at, :].astype(F32)
        scale = norm_scale(wide)
        by_a = acc[at, :].astype(BF).astype(F32)
        by_h = scale * by_a - wide * (scale * scale * scale * jnp.mean(by_a * wide, -1, keepdims=True))
        dh[at, :] = dh[at, :] + by_h.astype(BF)
        return 0

    def down_step(t, _):
        load_hid(t).wait()
        acc[0:hidden, :] += dot_t(hid[t % slots], dh[pl.ds(pl.multiple_of(t * TILE, TILE), TILE), :])

        @pl.when(t + slots < tiles)
        def _():
            load_hid(t + slots).start()

        return 0

    def zero():
        acc_gu[...] = jnp.zeros_like(acc_gu)

    def phase(p, _):
        part_of = p % 2
        lo = part_of * half

        @pl.when(p < first_down)
        def _():
            j = p // 2

            @pl.when(part_of == 0)
            def _():
                zero()
                acc_d[...] = jnp.zeros_like(acc_d)

            lax.fori_loop(lo, lo + half, wide_step(j, True), 0)

            @pl.when(part_of == 1)
            def _():
                grads(j)
                down = acc_d[...].T.astype(BF)
                for i in range(COLS // 16):
                    row = j * COLS + i * 16
                    device = row // rows_d
                    td[1, device // 2, device % 2, pl.ds(pl.multiple_of(row % rows_d, 16), 16), :] = down[i * 16 : i * 16 + 16, :]

            @pl.when(p == first_down - 1)
            def _():
                over_d(1).start()
                for c in later:
                    c.start()
                early[4].wait()
                lax.fori_loop(0, tiles, top_end, 0)

        @pl.when(jnp.logical_and(p >= first_down, p < first_low))
        def _():
            @pl.when(part_of == 0)
            def _():
                acc[0:hidden, :] = jnp.zeros((hidden, dim), F32)

            lax.fori_loop(part_of * (tiles // 2), part_of * (tiles // 2) + tiles // 2, down_step, 0)

            @pl.when(part_of == 1)
            def _():
                for b in range(nz):
                    for c in range(2):
                        k = (b * 2 + c) * rows_d
                        td[0, b, c] = acc[k : k + rows_d, :].astype(BF)
                over_d(0).start()
                for c in later:
                    c.wait()

        @pl.when(jnp.logical_and(p >= first_low, p < end_low))
        def _():
            j = (p - first_low) // 2

            @pl.when(part_of == 0)
            def _():
                zero()

            lax.fori_loop(lo, lo + half, wide_step(j, False), 0)

            @pl.when(part_of == 1)
            def _():
                grads(nf + j)

        events(p)
        return 0

    lax.fori_loop(0, end_low + WAIT + 1, phase, 0)

    all_ssq[me] = ssq[...]

    def scalar(k, slot):
        return pltpu.make_async_remote_copy(
            src_ref=ssq, dst_ref=all_ssq.at[slot], send_sem=q_send.at[k], recv_sem=q_recv.at[k],
            device_id={"dp": (me + k) % n}, device_id_type=MESH,
        )

    def tell(k, _):
        scalar(k, me).start()
        return 0

    lax.fori_loop(1, n, tell, 0)

    def told(k, _):
        scalar(k, (me + n - k) % n).wait()
        return 0

    lax.fori_loop(1, n, told, 0)
    total = jnp.sum(jnp.sum(jnp.sum(all_ssq[...], axis=0), axis=0, keepdims=True), axis=1, keepdims=True)
    count = 3 * 2 * dim * hidden
    factor[0, 0] = jnp.max(jnp.minimum(1.0, 0.5 * lax.rsqrt(total / count + 1e-30)))


def backward(n, h1, a1, dy, a0, hid, gu, dt):
    nz = n // 2
    tokens, dim = a0.shape
    hidden = dt.shape[2]
    nf, last = hidden // COLS, nz - 1
    rg, rd = dim // n, hidden // n
    anyspace, vmem = pl.BlockSpec(memory_space=pl.ANY), pl.BlockSpec(memory_space=pltpu.VMEM)
    V = lambda *s: pltpu.VMEM(s, BF)
    W = lambda *s: pltpu.VMEM(s, F32)
    S = lambda *s: pltpu.SemaphoreType.DMA(s)
    return pl.pallas_call(
        functools.partial(backward_kernel, n),
        out_shape=[
            jax.ShapeDtypeStruct((2, 2, rg, hidden), BF),
            jax.ShapeDtypeStruct((2, rd, dim), BF),
            jax.ShapeDtypeStruct((1, 1), F32),
        ],
        in_specs=[anyspace] * 7,
        out_specs=[vmem, vmem, pl.BlockSpec(memory_space=pltpu.SMEM)],
        scratch_shapes=[
            V(tokens, dim),
            V(tokens, dim),
            V(tokens, dim),
            W(tokens, dim),
            V(2, dim, hidden),
            V(nf, 2 * COLS, dim),
            V(dim, hidden),
            V(3, TILE, hidden),
            V(2 * nf, 2, nz, 2, rg, COLS),
            V(2, nz, 2, rd, dim),
            V(2 * nf, 2, nz, rg, COLS),
            V(2, nz, rd, dim),
            V(2 * nf - DIRECT, 2, last, 2, rg, COLS // 2),
            V(2, 2, last, rd, dim // 2),
            V(DIRECT, nz, 2, rg, COLS),
            W(dim, 2 * COLS),
            W(dim, COLS),
            W(8, 128),
            W(n, 8, 128),
            S(8),
            S(3),
            S(2 * nf + 2),
            S(2 * nf + 2),
            S(2 * nf, 2, last),
            S(2 * nf, 2, last),
            S(2, 2, last),
            S(2, 2, last),
            S(DIRECT, nz),
            S(DIRECT, nz),
            S(n),
            S(n),
        ],
        compiler_params=pltpu.CompilerParams(collective_id=1, has_side_effects=True, vmem_limit_bytes=VMEM_LIMIT),
        cost_estimate=pl.CostEstimate(flops=28 * tokens * dim * hidden, bytes_accessed=40 << 20, transcendentals=0),
        name="backward",
    )(h1, a1, dy, a0, hid, gu, dt)


def adamw(w, m, v, g):
    m = 0.9 * m + 0.1 * g
    v = 0.95 * v + 0.05 * g * g
    step = m * lax.rsqrt(v + 1e-8) + 0.1 * w
    return (w - 0.02 * step).astype(BF), m, v


def solution(mesh):
    n = mesh.shape["dp"]

    def step(x, dy, *arrays):
        weights, m, v = (arrays[i : i + 3] for i in (0, 3, 6))
        h1, a1, hid, a0, gu, dt = forward(n, x[0], *weights)
        sum_gu, sum_d, factor = backward(n, h1, a1, dy[0], a0, hid, gu, dt)
        gradients = [sum_gu[:, 0].astype(F32), sum_gu[:, 1].astype(F32), sum_d.astype(F32)]
        factor = factor[0, 0]
        new = [adamw(w.astype(F32), m, v, g * factor) for w, m, v, g in zip(weights, m, v, gradients, strict=True)]
        return tuple(one[which] for which in range(3) for one in new)

    states, cut = P(("rep", "dp"), None, None), P(None, "dp", None)
    return jax.shard_map(
        step,
        mesh=mesh,
        in_specs=(states, states) + (cut,) * 9,
        out_specs=(P("rep", "dp", None),) * 9,
        check_vma=False,
    )
```

```python
import functools

import jax
import jax.numpy as jnp
from jax import lax
from jax.experimental import pallas as pl
from jax.experimental.pallas import tpu as pltpu
from jax.sharding import PartitionSpec as P

MESH = pl.DeviceIdType.MESH
BF, F32 = jnp.bfloat16, jnp.float32
VMEM_LIMIT = 66_500_000
TILE = 512
WIDE = 1024
COLS = 256
DIRECT = 3
WAIT = 4


def dot(a, b):
    return jnp.dot(a, b, preferred_element_type=F32)


def dot_t(a, b):
    return lax.dot_general(a, b, (((0,), (0,)), ((), ())), preferred_element_type=F32)


def norm_scale(wide):
    return lax.rsqrt(jnp.mean(wide * wide, -1, keepdims=True) + 1e-6)


def places(n):
    nz = n // 2
    me = lax.axis_index("dp")
    z, core = me // 2, me % 2
    return me, z, core, ((z + 1) % nz) * 2 + core, ((z + nz - 1) % nz) * 2 + core, me + 1 - 2 * core


def barrier(devices):
    sem = pltpu.get_barrier_semaphore()
    for device in devices:
        pl.semaphore_signal(sem, inc=1, device_id={"dp": device}, device_id_type=MESH)
    pl.semaphore_wait(sem, len(devices))


def forward_kernel(n, x_hbm, wg_ref, wu_ref, wd_ref, h1_hbm, a1_hbm, hid_hbm, a0_hbm, gu_hbm, dt_hbm,
                   x, a0, hid, gu, d, dt, send_sem, recv_sem, in_sem, out_sem):
    nz = n // 2
    me, z, core, right, left, partner = places(n)
    tokens = x.shape[0]
    steps = tokens // TILE
    load = pltpu.make_async_copy(x_hbm, x, in_sem)
    load.start()
    barrier((right, left, partner))

    more, less = nz // 2, nz - 1 - nz // 2
    parts = [
        (wg_ref.at[0], gu, 0, more, less),
        (wu_ref.at[0], gu, 1, less, more),
        (wd_ref.at[0], d, 0, more, less),
        (wg_ref.at[1], gu, 2, less, more),
        (wu_ref.at[1], gu, 3, more, less),
        (wd_ref.at[1], d, 1, less, more),
    ]
    sent = []

    def block(i, chip, which):
        src, whole, first = parts[i][:3]
        rows = src.shape[0]
        return whole.at[first, pl.ds(pl.multiple_of((chip * 2 + which) * rows, 16), rows), :]

    def copy(i, k, src, dst, device):
        return pltpu.make_async_remote_copy(
            src_ref=src, dst_ref=dst, send_sem=send_sem.at[i, k], recv_sem=recv_sem.at[i, k],
            device_id={"dp": device}, device_id_type=MESH,
        )

    def send(i, k, src, dst, device):
        c = copy(i, k, src, dst, device)
        c.start()
        sent.append(c)

    def arrived(i, k, at):
        copy(i, k, at, at, partner).wait_recv()

    def begin(i):
        src, whole, first = parts[i][:3]
        rows = src.shape[0]
        own = block(i, z, core)
        send(i, 0, src, own, right)
        send(i, more, src, own, left)
        send(i, 2 * more, src, own, partner)
        whole[first, pl.ds(pl.multiple_of(me * rows, 16), rows), :] = src[...]

    def relay(i, s):
        hops_right, hops_left = parts[i][3:]
        if s <= hops_right:
            at = block(i, (z + nz - s) % nz, core)
            arrived(i, s - 1, at)
            if s < hops_right:
                send(i, s, at, at, right)
            send(i, 2 * more + s, at, at, partner)
        if s <= hops_left:
            at = block(i, (z + s) % nz, core)
            arrived(i, more + s - 1, at)
            if s < hops_left:
                send(i, more + s, at, at, left)
            send(i, 3 * more + s, at, at, partner)

    def finish(i):
        hops_right, hops_left = parts[i][3:]
        arrived(i, 2 * more, block(i, z, 1 - core))
        for s in range(1, hops_right + 1):
            arrived(i, 2 * more + s, block(i, (z + nz - s) % nz, 1 - core))
        for s in range(1, hops_left + 1):
            arrived(i, 3 * more + s, block(i, (z + s) % nz, 1 - core))

    outs = []

    def store(k, src, dst):
        c = pltpu.make_async_copy(src, dst, out_sem.at[k])
        c.start()
        outs.append(c)

    for i in range(3):
        begin(i)
    load.wait()

    def norm_step(t, _):
        at = pl.ds(pl.multiple_of(t * TILE, TILE), TILE)
        wide = x[at, :].astype(F32)
        a0[at, :] = (wide * norm_scale(wide)).astype(BF)
        return 0

    with jax.named_scope("gather0"):
        for s in range(1, more):
            if s < 3:
                lax.fori_loop((s - 1) * (steps // 2), s * (steps // 2), norm_step, 0)
            for i in range(3):
                relay(i, s)
        for i in range(3, 6):
            begin(i)
        relay(0, more)
        relay(1, more)
        finish(0)
        finish(1)
    store(0, a0, a0_hbm)

    def up_step(t, _):
        at = pl.ds(pl.multiple_of(t * TILE, TILE), TILE)
        a = a0[at, :]
        gate = dot(a, gu[0])
        up = dot(a, gu[1])
        hid[at, :] = (gate * jax.nn.sigmoid(gate) * up).astype(BF)
        return 0

    def down_step(t, _):
        at = pl.ds(pl.multiple_of(t * TILE, TILE), TILE)
        h = x[at, :] + dot(hid[at, :], d[0]).astype(BF)
        x[at, :] = h
        wide = h.astype(F32)
        a0[at, :] = (wide * norm_scale(wide)).astype(BF)
        return 0

    moves = [(2, 4), (3, 1), (4, 1), (5, 1), (3, 2), (4, 2), (5, 2), (3, 3), (4, 3), (5, 3), None, (3, 4), None, (4, 4), None, (5, 4)]
    each = steps // 8
    for q in range(8):
        with jax.named_scope("up"):
            lax.fori_loop(q * each, (q + 1) * each, up_step, 0)
        with jax.named_scope("move"):
            relay(*moves[q])
    store(1, hid, hid_hbm)
    store(2, gu.at[pl.ds(0, 2)], gu_hbm.at[pl.ds(0, 2)])
    outs[0].wait()
    finish(2)
    for q in range(8):
        with jax.named_scope("down"):
            lax.fori_loop(q * each, (q + 1) * each, down_step, 0)
        with jax.named_scope("move"):
            if moves[8 + q] is not None:
                relay(*moves[8 + q])
        if q == 0:
            dt[0] = d[0].T
            store(3, dt.at[0], dt_hbm.at[0])
    store(4, x, h1_hbm)
    store(7, a0, a1_hbm)
    with jax.named_scope("finish"):
        finish(3)
        finish(4)
    store(5, gu.at[pl.ds(2, 2)], gu_hbm.at[pl.ds(2, 2)])
    finish(5)
    dt[1] = d[1].T
    store(6, dt.at[1], dt_hbm.at[1])
    for c in sent:
        c.wait_send()
    for c in outs[1:]:
        c.wait()


def forward(n, x, wg, wu, wd):
    tokens, dim = x.shape
    hidden = wg.shape[2]
    anyspace, vmem = pl.BlockSpec(memory_space=pl.ANY), pl.BlockSpec(memory_space=pltpu.VMEM)
    shapes = [(tokens, dim), (tokens, dim), (tokens, hidden), (tokens, dim), (4, dim, hidden), (2, dim, hidden)]
    sems = 4 * (n // 4) + 1
    return pl.pallas_call(
        functools.partial(forward_kernel, n),
        out_shape=[jax.ShapeDtypeStruct(s, BF) for s in shapes],
        in_specs=[anyspace, vmem, vmem, vmem],
        out_specs=[anyspace] * 6,
        scratch_shapes=[
            pltpu.VMEM((tokens, dim), BF),
            pltpu.VMEM((tokens, dim), BF),
            pltpu.VMEM((tokens, hidden), BF),
            pltpu.VMEM((4, dim, hidden), BF),
            pltpu.VMEM((2, hidden, dim), BF),
            pltpu.VMEM((2, dim, hidden), BF),
            pltpu.SemaphoreType.DMA((6, sems)),
            pltpu.SemaphoreType.DMA((6, sems)),
            pltpu.SemaphoreType.DMA,
            pltpu.SemaphoreType.DMA((8,)),
        ],
        compiler_params=pltpu.CompilerParams(collective_id=0, has_side_effects=True, vmem_limit_bytes=VMEM_LIMIT),
        cost_estimate=pl.CostEstimate(flops=6 * tokens * dim * hidden, bytes_accessed=40 << 20, transcendentals=0),
        name="forward0",
    )(x, wg, wu, wd)


def backward_kernel(n, h1_hbm, a1_hbm, dy_hbm, a0_hbm, hid_hbm, gu_hbm, dt_hbm, sum_gu, sum_d, factor,
                    h1, a, dh, acc, gu, gt, dt, hid, tgu, td, pgu, pd, rgu, rd, rs, acc_gu, acc_d, ssq, all_ssq,
                    in_sem, hid_sem, p_send, p_recv, send_gu, recv_gu, send_d, recv_d, send_s, recv_s, q_send, q_recv):
    nz = n // 2
    me, z, core, right, left, partner = places(n)
    tokens, dim = a.shape
    hidden = dt.shape[1]
    nf = hidden // COLS
    last = nz - 1
    rows_g, rows_d = dim // n, hidden // n
    tiles, slots = tokens // TILE, hid.shape[0]
    half = tokens // WIDE // 2

    def load(k, src, dst):
        return pltpu.make_async_copy(src, dst, in_sem.at[k])

    def load_hid(t):
        slot = t % slots
        return pltpu.make_async_copy(hid_hbm.at[pl.ds(pl.multiple_of(t * TILE, TILE), TILE), :], hid.at[slot], hid_sem.at[slot])

    half_t = tokens // 2
    lo_t, hi_t = pl.ds(0, half_t), pl.ds(half_t, half_t)
    early = [
        load(0, gu_hbm.at[pl.ds(2, 2)], gu),
        load(1, dt_hbm.at[1], dt),
        load(2, a1_hbm.at[lo_t, :], a.at[lo_t, :]),
        load(3, dy_hbm.at[lo_t, :], dh.at[lo_t, :]),
    ]
    soon = [load(4, a1_hbm.at[hi_t, :], a.at[hi_t, :]), load(5, dy_hbm.at[hi_t, :], dh.at[hi_t, :])]
    whole_h1 = load(6, h1_hbm, h1)
    later = [load(7, a0_hbm, a), load(8, gu_hbm.at[pl.ds(0, 2)], gu), load(9, dt_hbm.at[0], dt)]
    for c in early:
        c.start()

    sem = pltpu.get_barrier_semaphore()
    for k in range(1, n):
        pl.semaphore_signal(sem, inc=1, device_id={"dp": (me + k) % n}, device_id_type=MESH)
    pl.semaphore_wait(sem, n - 1)

    ssq[...] = jnp.zeros_like(ssq)

    def begin_step(t, _):
        acc[pl.ds(pl.multiple_of(t * TILE, TILE), TILE), :] = jnp.zeros((TILE, dim), F32)
        return 0

    lax.fori_loop(0, tiles, begin_step, 0)
    early[0].wait()
    for j in range(nf):
        for i in range(2):
            gt[j, i * COLS : (i + 1) * COLS, :] = gu[i, :, j * COLS : (j + 1) * COLS].T
    for c in early[1:]:
        c.wait()
    for c in soon:
        c.start()

    def over_gu(q):
        return pltpu.make_async_remote_copy(
            src_ref=tgu.at[q, :, :, 1 - core], dst_ref=pgu.at[q], send_sem=p_send.at[q], recv_sem=p_recv.at[q],
            device_id={"dp": partner}, device_id_type=MESH,
        )

    def over_d(layer):
        k = 2 * nf + layer
        return pltpu.make_async_remote_copy(
            src_ref=td.at[layer, :, 1 - core], dst_ref=pd.at[layer], send_sem=p_send.at[k], recv_sem=p_recv.at[k],
            device_id={"dp": partner}, device_id_type=MESH,
        )

    def chip(way, s):
        return (z + 2 * nz - 1 - s) % nz if way == 0 else (z + 1 + s) % nz

    def squared(v):
        g = v.astype(F32)
        g = g * g
        while g.ndim > 2:
            g = jnp.sum(g, axis=0)
        g = jnp.sum(g, axis=0, keepdims=True)
        total = g[:, 0:128]
        for k in range(1, g.shape[1] // 128):
            total = total + g[:, k * 128 : (k + 1) * 128]
        ssq[0:1, :] += total

    class Gu:
        def __init__(self, q):
            self.q = q

        def over(self):
            return over_gu(self.q)

        def cols(self, way):
            return slice(way * (COLS // 2), (way + 1) * (COLS // 2))

        def term(self, way, b):
            return tgu[self.q, :, b, core, :, self.cols(way)].astype(F32) + pgu[self.q, :, b, :, self.cols(way)].astype(F32)

        def keep(self, way, b, v):
            tgu[self.q, :, b, core, :, self.cols(way)] = v

        def got(self, way, s):
            return rgu[self.q, way, s].astype(F32)

        def move(self, way, s):
            return pltpu.make_async_remote_copy(
                src_ref=tgu.at[self.q, :, chip(way, s), core, :, pl.ds(way * (COLS // 2), COLS // 2)], dst_ref=rgu.at[self.q, way, s],
                send_sem=send_gu.at[self.q, way, s], recv_sem=recv_gu.at[self.q, way, s],
                device_id={"dp": right if way == 0 else left}, device_id_type=MESH,
            )

        def put(self, way, v):
            layer, j = 1 - self.q // nf, self.q % nf
            w = COLS // 2
            sum_gu[layer, :, :, pl.ds(pl.multiple_of(j * COLS + way * w, w), w)] = v

    class Down:
        def __init__(self, layer):
            self.layer = layer

        def over(self):
            return over_d(self.layer)

        def cols(self, way):
            return slice(way * (dim // 2), (way + 1) * (dim // 2))

        def term(self, way, b):
            return td[self.layer, b, core, :, self.cols(way)].astype(F32) + pd[self.layer, b, :, self.cols(way)].astype(F32)

        def keep(self, way, b, v):
            td[self.layer, b, core, :, self.cols(way)] = v

        def got(self, way, s):
            return rd[self.layer, way, s].astype(F32)

        def move(self, way, s):
            return pltpu.make_async_remote_copy(
                src_ref=td.at[self.layer, chip(way, s), core, :, pl.ds(way * (dim // 2), dim // 2)], dst_ref=rd.at[self.layer, way, s],
                send_sem=send_d.at[self.layer, way, s], recv_sem=recv_d.at[self.layer, way, s],
                device_id={"dp": right if way == 0 else left}, device_id_type=MESH,
            )

        def put(self, way, v):
            sum_d[self.layer, :, self.cols(way)] = v

    def event(part, s):
        @pl.when(s == 0)
        def _():
            part.over().wait()
            for way in range(2):
                part.keep(way, chip(way, s), part.term(way, chip(way, s)).astype(BF))
            for way in range(2):
                part.move(way, s).start()

        @pl.when(jnp.logical_and(s > 0, s < last))
        def _():
            for way in range(2):
                part.move(way, s - 1).wait()
                part.keep(way, chip(way, s), (part.got(way, s - 1) + part.term(way, chip(way, s))).astype(BF))
                part.move(way, s).start()

        @pl.when(s == last)
        def _():
            for way in range(2):
                part.move(way, s - 1).wait()
                v = (part.got(way, s - 1) + part.term(way, chip(way, s))).astype(BF)
                part.put(way, v)
                squared(v)

    first_top, first_down, first_low = 0, 2 * nf, 2 * nf + 2
    end_low = first_low + 2 * nf

    def ready(q):
        return 2 * (q + q // nf)

    rings = 2 * nf - DIRECT
    order = sorted(range(1, nz), key=lambda k: -min(k, nz - k))

    def straight(i, k):
        to = (z + k) % nz
        return pltpu.make_async_remote_copy(
            src_ref=tgu.at[rings + i, :, to, core], dst_ref=rs.at[i, k], send_sem=send_s.at[i, k], recv_sem=recv_s.at[i, k],
            device_id={"dp": to * 2 + core}, device_id_type=MESH,
        )

    def both_terms(q, b):
        return tgu[q, :, b, core].astype(F32) + pgu[q, :, b].astype(F32)

    def events(p):
        def each_direct(i, _):
            q = rings + i
            s = p - (ready(q) + 2)

            @pl.when(s == 0)
            def _():
                with jax.named_scope("over"):
                    over_gu(q).wait()
                for k in order:
                    to = (z + k) % nz
                    tgu[q, :, to, core] = both_terms(q, to).astype(BF)
                    straight(i, k).start()

            @pl.when(s == WAIT)
            def _():
                v = both_terms(q, z)
                with jax.named_scope("direct"):
                    for k in range(1, nz):
                        straight(i, k).wait()
                for k in range(1, nz):
                    v = v + rs[i, k].astype(F32)
                v = v.astype(BF)
                sum_gu[0, :, :, pl.ds(pl.multiple_of((q - nf) * COLS, COLS), COLS)] = v
                squared(v)

            return 0

        def each_gu(q, _):
            s = p - (ready(q) + 2)

            @pl.when(jnp.logical_and(s >= 0, s <= last))
            def _():
                event(Gu(q), s)

            return 0

        def each_d(k, _):
            s = p - (first_down + 2 * k)

            @pl.when(jnp.logical_and(s >= 0, s <= last))
            def _():
                event(Down(1 - k), s)

            return 0

        @pl.when(p >= ready(rings) + 2)
        def _():
            lax.fori_loop(0, DIRECT, each_direct, 0)

        @pl.when(p >= first_down)
        def _():
            lax.fori_loop(0, 2, each_d, 0)

        lax.fori_loop(0, rings, each_gu, 0)

    def grads(q):
        for b in range(nz):
            for c in range(2):
                k = (b * 2 + c) * rows_g
                for i in range(2):
                    tgu[q, i, b, c] = acc_gu[k : k + rows_g, i * COLS : (i + 1) * COLS].astype(BF)
        over_gu(q).start()

    def wide_step(j, with_top):
        cols = pl.ds(pl.multiple_of(j * COLS, COLS), COLS)

        def body(t, _):
            at = pl.ds(pl.multiple_of(t * WIDE, WIDE), WIDE)
            rows = a[at, :]
            by_y = dh[at, :]
            gate = dot(rows, gu[0, :, cols])
            up = dot(rows, gu[1, :, cols])
            by_hid = dot(by_y, dt[:, cols]).astype(BF).astype(F32)
            sig = jax.nn.sigmoid(gate)
            act = gate * sig
            by_up = (by_hid * act).astype(BF)
            by_gate = (by_hid * up * (sig + act * (1.0 - sig))).astype(BF)
            by_both = jnp.concatenate([by_gate, by_up], axis=1)
            acc_gu[...] += dot_t(rows, by_both)
            if with_top:
                acc_d[...] += dot_t(by_y, (act * up).astype(BF))
                acc[at, :] += dot(by_both, gt[j])
            return 0

        return body

    def top_end(t, _):
        at = pl.ds(pl.multiple_of(t * TILE, TILE), TILE)
        wide = h1[at, :].astype(F32)
        scale = norm_scale(wide)
        by_a = acc[at, :].astype(BF).astype(F32)
        by_h = scale * by_a - wide * (scale * scale * scale * jnp.mean(by_a * wide, -1, keepdims=True))
        dh[at, :] = dh[at, :] + by_h.astype(BF)
        return 0

    def down_step(t, _):
        load_hid(t).wait()
        acc[0:hidden, :] += dot_t(hid[t % slots], dh[pl.ds(pl.multiple_of(t * TILE, TILE), TILE), :])

        @pl.when(t + slots < tiles)
        def _():
            load_hid(t + slots).start()

        return 0

    def zero():
        acc_gu[...] = jnp.zeros_like(acc_gu)

    def phase(p, _):
        part_of = p % 2
        lo = part_of * half

        @pl.when(p < first_down)
        def _():
            j = p // 2

            @pl.when(p == 1)
            def _():
                for c in soon:
                    c.wait()
                whole_h1.start()
                for t in range(slots):
                    load_hid(t).start()

            @pl.when(part_of == 0)
            def _():
                zero()
                acc_d[...] = jnp.zeros_like(acc_d)

            with jax.named_scope("top"):
                lax.fori_loop(lo, lo + half, wide_step(j, True), 0)

            @pl.when(part_of == 1)
            def _():
                grads(j)
                down = acc_d[...].T.astype(BF)
                for i in range(COLS // 16):
                    row = j * COLS + i * 16
                    device = row // rows_d
                    td[1, device // 2, device % 2, pl.ds(pl.multiple_of(row % rows_d, 16), 16), :] = down[i * 16 : i * 16 + 16, :]

            @pl.when(p == first_down - 1)
            def _():
                over_d(1).start()
                for c in later:
                    c.start()
                whole_h1.wait()
                with jax.named_scope("topend"):
                    lax.fori_loop(0, tiles, top_end, 0)

        @pl.when(jnp.logical_and(p >= first_down, p < first_low))
        def _():
            @pl.when(part_of == 0)
            def _():
                acc[0:hidden, :] = jnp.zeros((hidden, dim), F32)

            lax.fori_loop(part_of * (tiles // 2), part_of * (tiles // 2) + tiles // 2, down_step, 0)

            @pl.when(part_of == 1)
            def _():
                for b in range(nz):
                    for c in range(2):
                        k = (b * 2 + c) * rows_d
                        td[0, b, c] = acc[k : k + rows_d, :].astype(BF)
                over_d(0).start()
                for c in later:
                    c.wait()

        @pl.when(jnp.logical_and(p >= first_low, p < end_low))
        def _():
            j = (p - first_low) // 2

            @pl.when(part_of == 0)
            def _():
                zero()

            with jax.named_scope("low"):
                lax.fori_loop(lo, lo + half, wide_step(j, False), 0)

            @pl.when(part_of == 1)
            def _():
                grads(nf + j)

        with jax.named_scope("events"):
            events(p)
        return 0

    lax.fori_loop(0, end_low + WAIT + 1, phase, 0)

    all_ssq[me] = ssq[...]

    def scalar(k, slot):
        return pltpu.make_async_remote_copy(
            src_ref=ssq, dst_ref=all_ssq.at[slot], send_sem=q_send.at[k], recv_sem=q_recv.at[k],
            device_id={"dp": (me + k) % n}, device_id_type=MESH,
        )

    def tell(k, _):
        scalar(k, me).start()
        return 0

    lax.fori_loop(1, n, tell, 0)

    def told(k, _):
        scalar(k, (me + n - k) % n).wait()
        return 0

    with jax.named_scope("told"):
        lax.fori_loop(1, n, told, 0)
    total = jnp.sum(jnp.sum(jnp.sum(all_ssq[...], axis=0), axis=0, keepdims=True), axis=1, keepdims=True)
    count = 3 * 2 * dim * hidden
    factor[0, 0] = jnp.max(jnp.minimum(1.0, 0.5 * lax.rsqrt(total / count + 1e-30)))


def backward(n, h1, a1, dy, a0, hid, gu, dt):
    nz = n // 2
    tokens, dim = a0.shape
    hidden = dt.shape[2]
    nf, last = hidden // COLS, nz - 1
    rg, rd = dim // n, hidden // n
    anyspace, vmem = pl.BlockSpec(memory_space=pl.ANY), pl.BlockSpec(memory_space=pltpu.VMEM)
    V = lambda *s: pltpu.VMEM(s, BF)
    W = lambda *s: pltpu.VMEM(s, F32)
    S = lambda *s: pltpu.SemaphoreType.DMA(s)
    return pl.pallas_call(
        functools.partial(backward_kernel, n),
        out_shape=[
            jax.ShapeDtypeStruct((2, 2, rg, hidden), BF),
            jax.ShapeDtypeStruct((2, rd, dim), BF),
            jax.ShapeDtypeStruct((1, 1), F32),
        ],
        in_specs=[anyspace] * 7,
        out_specs=[vmem, vmem, pl.BlockSpec(memory_space=pltpu.SMEM)],
        scratch_shapes=[
            V(tokens, dim),
            V(tokens, dim),
            V(tokens, dim),
            W(tokens, dim),
            V(2, dim, hidden),
            V(nf, 2 * COLS, dim),
            V(dim, hidden),
            V(3, TILE, hidden),
            V(2 * nf, 2, nz, 2, rg, COLS),
            V(2, nz, 2, rd, dim),
            V(2 * nf, 2, nz, rg, COLS),
            V(2, nz, rd, dim),
            V(2 * nf - DIRECT, 2, last, 2, rg, COLS // 2),
            V(2, 2, last, rd, dim // 2),
            V(DIRECT, nz, 2, rg, COLS),
            W(dim, 2 * COLS),
            W(dim, COLS),
            W(8, 128),
            W(n, 8, 128),
            S(10),
            S(3),
            S(2 * nf + 2),
            S(2 * nf + 2),
            S(2 * nf, 2, last),
            S(2 * nf, 2, last),
            S(2, 2, last),
            S(2, 2, last),
            S(DIRECT, nz),
            S(DIRECT, nz),
            S(n),
            S(n),
        ],
        compiler_params=pltpu.CompilerParams(collective_id=1, has_side_effects=True, vmem_limit_bytes=61_000_000),
        cost_estimate=pl.CostEstimate(flops=28 * tokens * dim * hidden, bytes_accessed=40 << 20, transcendentals=0),
        name="backward",
    )(h1, a1, dy, a0, hid, gu, dt)


def adamw(w, m, v, g):
    m = 0.9 * m + 0.1 * g
    v = 0.95 * v + 0.05 * g * g
    step = m * lax.rsqrt(v + 1e-8) + 0.1 * w
    return (w - 0.02 * step).astype(BF), m, v


def solution(mesh):
    n = mesh.shape["dp"]

    def step(x, dy, *arrays):
        weights, m, v = (arrays[i : i + 3] for i in (0, 3, 6))
        h1, a1, hid, a0, gu, dt = forward(n, x[0], *weights)
        sum_gu, sum_d, factor = backward(n, h1, a1, dy[0], a0, hid, gu, dt)
        gradients = [sum_gu[:, 0].astype(F32), sum_gu[:, 1].astype(F32), sum_d.astype(F32)]
        factor = factor[0, 0]
        new = [adamw(w.astype(F32), m, v, g * factor) for w, m, v, g in zip(weights, m, v, gradients, strict=True)]
        return tuple(one[which] for which in range(3) for one in new)

    states, cut = P(("rep", "dp"), None, None), P(None, "dp", None)
    return jax.shard_map(
        step,
        mesh=mesh,
        in_specs=(states, states) + (cut,) * 9,
        out_specs=(P("rep", "dp", None),) * 9,
        check_vma=False,
    )
```

```python
import functools

import jax
import jax.numpy as jnp
from jax import lax
from jax.experimental import pallas as pl
from jax.experimental.pallas import tpu as pltpu
from jax.sharding import PartitionSpec as P

MESH = pl.DeviceIdType.MESH
BF, F32 = jnp.bfloat16, jnp.float32
VMEM_LIMIT = 66_500_000
TILE = 512
WIDE = 1024
COLS = 256


def dot(a, b):
    return jnp.dot(a, b, preferred_element_type=F32)


def dot_t(a, b):
    return lax.dot_general(a, b, (((0,), (0,)), ((), ())), preferred_element_type=F32)


def norm_scale(wide):
    return lax.rsqrt(jnp.mean(wide * wide, -1, keepdims=True) + 1e-6)


def places(n):
    nz = n // 2
    me = lax.axis_index("dp")
    z, core = me // 2, me % 2
    return me, z, core, ((z + 1) % nz) * 2 + core, ((z + nz - 1) % nz) * 2 + core, me + 1 - 2 * core


def barrier(devices):
    sem = pltpu.get_barrier_semaphore()
    for device in devices:
        pl.semaphore_signal(sem, inc=1, device_id={"dp": device}, device_id_type=MESH)
    pl.semaphore_wait(sem, len(devices))


def forward_kernel(n, x_hbm, wg_ref, wu_ref, wd_ref, h1_hbm, a1_hbm, hid_hbm, a0_hbm, gu_hbm, dt_hbm,
                   x, a0, hid, gu, d, dt, send_sem, recv_sem, in_sem, out_sem):
    nz = n // 2
    me, z, core, right, left, partner = places(n)
    tokens = x.shape[0]
    steps = tokens // TILE
    load = pltpu.make_async_copy(x_hbm, x, in_sem)
    load.start()
    barrier((right, left, partner))

    more, less = nz // 2, nz - 1 - nz // 2
    parts = [
        (wg_ref.at[0], gu, 0, more, less),
        (wu_ref.at[0], gu, 1, less, more),
        (wd_ref.at[0], d, 0, more, less),
        (wg_ref.at[1], gu, 2, less, more),
        (wu_ref.at[1], gu, 3, more, less),
        (wd_ref.at[1], d, 1, less, more),
    ]
    sent = []

    def block(i, chip, which):
        src, whole, first = parts[i][:3]
        rows = src.shape[0]
        return whole.at[first, pl.ds(pl.multiple_of((chip * 2 + which) * rows, 16), rows), :]

    def copy(i, k, src, dst, device):
        return pltpu.make_async_remote_copy(
            src_ref=src, dst_ref=dst, send_sem=send_sem.at[i, k], recv_sem=recv_sem.at[i, k],
            device_id={"dp": device}, device_id_type=MESH,
        )

    def send(i, k, src, dst, device):
        c = copy(i, k, src, dst, device)
        c.start()
        sent.append(c)

    def arrived(i, k, at):
        copy(i, k, at, at, partner).wait_recv()

    def begin(i):
        src, whole, first = parts[i][:3]
        rows = src.shape[0]
        own = block(i, z, core)
        send(i, 0, src, own, right)
        send(i, more, src, own, left)
        send(i, 2 * more, src, own, partner)
        whole[first, pl.ds(pl.multiple_of(me * rows, 16), rows), :] = src[...]

    def relay(i, s):
        hops_right, hops_left = parts[i][3:]
        if s <= hops_right:
            at = block(i, (z + nz - s) % nz, core)
            arrived(i, s - 1, at)
            if s < hops_right:
                send(i, s, at, at, right)
            send(i, 2 * more + s, at, at, partner)
        if s <= hops_left:
            at = block(i, (z + s) % nz, core)
            arrived(i, more + s - 1, at)
            if s < hops_left:
                send(i, more + s, at, at, left)
            send(i, 3 * more + s, at, at, partner)

    def finish(i):
        hops_right, hops_left = parts[i][3:]
        arrived(i, 2 * more, block(i, z, 1 - core))
        for s in range(1, hops_right + 1):
            arrived(i, 2 * more + s, block(i, (z + nz - s) % nz, 1 - core))
        for s in range(1, hops_left + 1):
            arrived(i, 3 * more + s, block(i, (z + s) % nz, 1 - core))

    outs = []

    def store(k, src, dst):
        c = pltpu.make_async_copy(src, dst, out_sem.at[k])
        c.start()
        outs.append(c)

    for i in range(3):
        begin(i)
    load.wait()

    def norm_step(t, _):
        at = pl.ds(pl.multiple_of(t * TILE, TILE), TILE)
        wide = x[at, :].astype(F32)
        a0[at, :] = (wide * norm_scale(wide)).astype(BF)
        return 0

    with jax.named_scope("gather0"):
        for s in range(1, more):
            if s < 3:
                lax.fori_loop((s - 1) * (steps // 2), s * (steps // 2), norm_step, 0)
            for i in range(3):
                relay(i, s)
        for i in range(3, 6):
            begin(i)
        relay(0, more)
        relay(1, more)
        finish(0)
        finish(1)
    store(0, a0, a0_hbm)

    def up_step(t, _):
        at = pl.ds(pl.multiple_of(t * TILE, TILE), TILE)
        a = a0[at, :]
        gate = dot(a, gu[0])
        up = dot(a, gu[1])
        hid[at, :] = (gate * jax.nn.sigmoid(gate) * up).astype(BF)
        return 0

    def down_step(t, _):
        at = pl.ds(pl.multiple_of(t * TILE, TILE), TILE)
        h = x[at, :] + dot(hid[at, :], d[0]).astype(BF)
        x[at, :] = h
        wide = h.astype(F32)
        a0[at, :] = (wide * norm_scale(wide)).astype(BF)
        return 0

    moves = [(2, 4), (3, 1), (4, 1), (5, 1), (3, 2), (4, 2), (5, 2), (3, 3), (4, 3), (5, 3), None, (3, 4), None, (4, 4), None, (5, 4)]
    each = steps // 8
    for q in range(8):
        with jax.named_scope("up"):
            lax.fori_loop(q * each, (q + 1) * each, up_step, 0)
        with jax.named_scope("move"):
            relay(*moves[q])
    store(1, hid, hid_hbm)
    store(2, gu.at[pl.ds(0, 2)], gu_hbm.at[pl.ds(0, 2)])
    outs[0].wait()
    finish(2)
    for q in range(8):
        with jax.named_scope("down"):
            lax.fori_loop(q * each, (q + 1) * each, down_step, 0)
        with jax.named_scope("move"):
            if moves[8 + q] is not None:
                relay(*moves[8 + q])
        at = pl.ds(q * each * TILE, each * TILE)
        store(6 + 2 * q, x.at[at, :], h1_hbm.at[at, :])
        store(7 + 2 * q, a0.at[at, :], a1_hbm.at[at, :])
        if q == 0:
            dt[0] = d[0].T
            store(3, dt.at[0], dt_hbm.at[0])
    with jax.named_scope("finish"):
        finish(3)
        finish(4)
    store(5, gu.at[pl.ds(2, 2)], gu_hbm.at[pl.ds(2, 2)])
    finish(5)
    dt[1] = d[1].T
    store(4, dt.at[1], dt_hbm.at[1])
    for c in sent:
        c.wait_send()
    for c in outs[1:]:
        c.wait()


def forward(n, x, wg, wu, wd):
    tokens, dim = x.shape
    hidden = wg.shape[2]
    anyspace, vmem = pl.BlockSpec(memory_space=pl.ANY), pl.BlockSpec(memory_space=pltpu.VMEM)
    shapes = [(tokens, dim), (tokens, dim), (tokens, hidden), (tokens, dim), (4, dim, hidden), (2, dim, hidden)]
    sems = 4 * (n // 4) + 1
    return pl.pallas_call(
        functools.partial(forward_kernel, n),
        out_shape=[jax.ShapeDtypeStruct(s, BF) for s in shapes],
        in_specs=[anyspace, vmem, vmem, vmem],
        out_specs=[anyspace] * 6,
        scratch_shapes=[
            pltpu.VMEM((tokens, dim), BF),
            pltpu.VMEM((tokens, dim), BF),
            pltpu.VMEM((tokens, hidden), BF),
            pltpu.VMEM((4, dim, hidden), BF),
            pltpu.VMEM((2, hidden, dim), BF),
            pltpu.VMEM((2, dim, hidden), BF),
            pltpu.SemaphoreType.DMA((6, sems)),
            pltpu.SemaphoreType.DMA((6, sems)),
            pltpu.SemaphoreType.DMA,
            pltpu.SemaphoreType.DMA((22,)),
        ],
        compiler_params=pltpu.CompilerParams(collective_id=0, has_side_effects=True, vmem_limit_bytes=VMEM_LIMIT),
        cost_estimate=pl.CostEstimate(flops=6 * tokens * dim * hidden, bytes_accessed=40 << 20, transcendentals=0),
        name="forward0",
    )(x, wg, wu, wd)


def backward_kernel(n, h1_hbm, a1_hbm, dy_hbm, a0_hbm, hid_hbm, gu_hbm, dt_hbm, out_gu, out_d, factor,
                    h1, a, dh, acc, gu, gt, dt, hid, tgu, td, pgu, pd, rgu, rd, sum_gu, sum_d, acc_gu, acc_d, ssq, all_ssq,
                    in_sem, hid_sem, p_send, p_recv, send_gu, recv_gu, send_d, recv_d, q_send, q_recv):
    nz = n // 2
    me, z, core, right, left, partner = places(n)
    tokens, dim = a.shape
    hidden = dt.shape[1]
    nf = hidden // COLS
    far, near = nz // 2, nz - 1 - nz // 2
    rows_g, rows_d = dim // n, hidden // n
    tiles, slots = tokens // TILE, hid.shape[0]
    half = tokens // WIDE // 2

    def load(k, src, dst):
        return pltpu.make_async_copy(src, dst, in_sem.at[k])

    def load_hid(t):
        slot = t % slots
        return pltpu.make_async_copy(hid_hbm.at[pl.ds(pl.multiple_of(t * TILE, TILE), TILE), :], hid.at[slot], hid_sem.at[slot])

    half_t = tokens // 2
    lo_t, hi_t = pl.ds(0, half_t), pl.ds(half_t, half_t)
    early = [
        load(0, gu_hbm.at[pl.ds(2, 2)], gu),
        load(1, dt_hbm.at[1], dt),
        load(2, a1_hbm.at[lo_t, :], a.at[lo_t, :]),
        load(3, dy_hbm.at[lo_t, :], dh.at[lo_t, :]),
    ]
    soon = [load(4, a1_hbm.at[hi_t, :], a.at[hi_t, :]), load(5, dy_hbm.at[hi_t, :], dh.at[hi_t, :])]
    whole_h1 = load(6, h1_hbm, h1)
    later = [load(7, a0_hbm, a), load(8, gu_hbm.at[pl.ds(0, 2)], gu), load(9, dt_hbm.at[0], dt)]
    for c in early:
        c.start()

    sem = pltpu.get_barrier_semaphore()
    for k in range(1, n):
        pl.semaphore_signal(sem, inc=1, device_id={"dp": (me + k) % n}, device_id_type=MESH)
    pl.semaphore_wait(sem, n - 1)

    ssq[...] = jnp.zeros_like(ssq)

    def begin_step(t, _):
        acc[pl.ds(pl.multiple_of(t * TILE, TILE), TILE), :] = jnp.zeros((TILE, dim), F32)
        return 0

    lax.fori_loop(0, tiles, begin_step, 0)
    early[0].wait()
    for j in range(nf):
        for i in range(2):
            gt[j, i * COLS : (i + 1) * COLS, :] = gu[i, :, j * COLS : (j + 1) * COLS].T
    for c in early[1:]:
        c.wait()
    for c in soon:
        c.start()

    def over_gu(q):
        return pltpu.make_async_remote_copy(
            src_ref=tgu.at[q, :, :, 1 - core], dst_ref=pgu.at[q], send_sem=p_send.at[q], recv_sem=p_recv.at[q],
            device_id={"dp": partner}, device_id_type=MESH,
        )

    def over_d(layer):
        k = 2 * nf + layer
        return pltpu.make_async_remote_copy(
            src_ref=td.at[layer, :, 1 - core], dst_ref=pd.at[layer], send_sem=p_send.at[k], recv_sem=p_recv.at[k],
            device_id={"dp": partner}, device_id_type=MESH,
        )

    def sides(odd):
        sign = 1 - 2 * odd

        def chip(way, s):
            return (z + 2 * nz + sign * (far - s)) % nz if way == 0 else (z + 2 * nz - sign * (near - s)) % nz

        def device(way):
            return ((z + nz + (sign if way == 0 else -sign)) % nz) * 2 + core

        return chip, device

    def squared(v):
        g = v.astype(F32)
        g = g * g
        while g.ndim > 2:
            g = jnp.sum(g, axis=0)
        g = jnp.sum(g, axis=0, keepdims=True)
        total = g[:, 0:128]
        for k in range(1, g.shape[1] // 128):
            total = total + g[:, k * 128 : (k + 1) * 128]
        ssq[0:1, :] += total

    class Gu:
        def __init__(self, q):
            self.q = q
            self.chip, self.device = sides(q % 2)

        def over(self):
            return over_gu(self.q)

        def term(self, b):
            return tgu[self.q, :, b, core].astype(F32) + pgu[self.q, :, b].astype(F32)

        def keep(self, b, v):
            tgu[self.q, :, b, core] = v

        def got(self, way, s):
            return rgu[self.q, way, s].astype(F32)

        def move(self, way, s):
            return pltpu.make_async_remote_copy(
                src_ref=tgu.at[self.q, :, self.chip(way, s), core], dst_ref=rgu.at[self.q, way, s],
                send_sem=send_gu.at[self.q, way, s], recv_sem=recv_gu.at[self.q, way, s],
                device_id={"dp": self.device(way)}, device_id_type=MESH,
            )

        def put(self, v):
            layer, j = 1 - self.q // nf, self.q % nf
            sum_gu[layer, :, :, pl.ds(pl.multiple_of(j * COLS, COLS), COLS)] = v

    class Down:
        def __init__(self, layer):
            self.layer = layer
            self.chip, self.device = sides(layer)

        def over(self):
            return over_d(self.layer)

        def term(self, b):
            return td[self.layer, b, core].astype(F32) + pd[self.layer, b].astype(F32)

        def keep(self, b, v):
            td[self.layer, b, core] = v

        def got(self, way, s):
            return rd[self.layer, way, s].astype(F32)

        def move(self, way, s):
            return pltpu.make_async_remote_copy(
                src_ref=td.at[self.layer, self.chip(way, s), core], dst_ref=rd.at[self.layer, way, s],
                send_sem=send_d.at[self.layer, way, s], recv_sem=recv_d.at[self.layer, way, s],
                device_id={"dp": self.device(way)}, device_id_type=MESH,
            )

        def put(self, v):
            sum_d[self.layer] = v

    def event(part, s):
        def on(way):
            b = part.chip(way, s)
            part.move(way, s - 1).wait()
            part.keep(b, (part.got(way, s - 1) + part.term(b)).astype(BF))
            part.move(way, s).start()

        @pl.when(s == 0)
        def _():
            part.over().wait()
            for way in range(2):
                b = part.chip(way, s)
                part.keep(b, part.term(b).astype(BF))
            for way in range(2):
                part.move(way, s).start()

        @pl.when(jnp.logical_and(s > 0, s < far))
        def _():
            on(0)

        @pl.when(jnp.logical_and(s > 0, s < near))
        def _():
            on(1)

        @pl.when(s == far)
        def _():
            part.move(0, far - 1).wait()
            part.move(1, near - 1).wait()
            v = (part.term(z) + part.got(0, far - 1) + part.got(1, near - 1)).astype(BF)
            part.put(v)
            squared(v)

    first_top, first_down, first_low = 0, 2 * nf, 2 * nf + 2
    end_low = first_low + 2 * nf

    def ready(q):
        return 2 * (q + q // nf)

    def events(p):
        def each_gu(q, _):
            s = p - (ready(q) + 2)

            @pl.when(jnp.logical_and(s >= 0, s <= far))
            def _():
                event(Gu(q), s)

            return 0

        def each_d(k, _):
            s = p - (first_down + 2 * k)

            @pl.when(jnp.logical_and(s >= 0, s <= far))
            def _():
                event(Down(1 - k), s)

            return 0

        @pl.when(jnp.logical_and(p >= first_down, p < first_down + far + 3))
        def _():
            lax.fori_loop(0, 2, each_d, 0)

        lax.fori_loop(0, 2 * nf, each_gu, 0)

    def grads(q):
        for b in range(nz):
            for c in range(2):
                k = (b * 2 + c) * rows_g
                for i in range(2):
                    tgu[q, i, b, c] = acc_gu[k : k + rows_g, i * COLS : (i + 1) * COLS].astype(BF)
        over_gu(q).start()

    def wide_step(j, with_top):
        cols = pl.ds(pl.multiple_of(j * COLS, COLS), COLS)

        def body(t, _):
            at = pl.ds(pl.multiple_of(t * WIDE, WIDE), WIDE)
            rows = a[at, :]
            by_y = dh[at, :]
            gate = dot(rows, gu[0, :, cols])
            up = dot(rows, gu[1, :, cols])
            by_hid = dot(by_y, dt[:, cols]).astype(BF).astype(F32)
            sig = jax.nn.sigmoid(gate)
            act = gate * sig
            by_up = (by_hid * act).astype(BF)
            by_gate = (by_hid * up * (sig + act * (1.0 - sig))).astype(BF)
            by_both = jnp.concatenate([by_gate, by_up], axis=1)
            acc_gu[...] += dot_t(rows, by_both)
            if with_top:
                acc_d[...] += dot_t(by_y, (act * up).astype(BF))
                acc[at, :] += dot(by_both, gt[j])
            return 0

        return body

    def top_end(t, _):
        at = pl.ds(pl.multiple_of(t * TILE, TILE), TILE)
        wide = h1[at, :].astype(F32)
        scale = norm_scale(wide)
        by_a = acc[at, :].astype(BF).astype(F32)
        by_h = scale * by_a - wide * (scale * scale * scale * jnp.mean(by_a * wide, -1, keepdims=True))
        dh[at, :] = dh[at, :] + by_h.astype(BF)
        return 0

    def down_step(t, _):
        load_hid(t).wait()
        acc[0:hidden, :] += dot_t(hid[t % slots], dh[pl.ds(pl.multiple_of(t * TILE, TILE), TILE), :])

        @pl.when(t + slots < tiles)
        def _():
            load_hid(t + slots).start()

        return 0

    def zero():
        acc_gu[...] = jnp.zeros_like(acc_gu)

    def phase(p, _):
        part_of = p % 2
        lo = part_of * half

        @pl.when(p < first_down)
        def _():
            j = p // 2

            @pl.when(p == 1)
            def _():
                for c in soon:
                    c.wait()
                whole_h1.start()
                for t in range(slots):
                    load_hid(t).start()

            @pl.when(part_of == 0)
            def _():
                zero()
                acc_d[...] = jnp.zeros_like(acc_d)

            with jax.named_scope("top"):
                lax.fori_loop(lo, lo + half, wide_step(j, True), 0)

            @pl.when(part_of == 1)
            def _():
                grads(j)
                down = acc_d[...].T.astype(BF)
                for i in range(COLS // 16):
                    row = j * COLS + i * 16
                    device = row // rows_d
                    td[1, device // 2, device % 2, pl.ds(pl.multiple_of(row % rows_d, 16), 16), :] = down[i * 16 : i * 16 + 16, :]

            @pl.when(p == first_down - 1)
            def _():
                over_d(1).start()
                for c in later:
                    c.start()
                whole_h1.wait()
                with jax.named_scope("topend"):
                    lax.fori_loop(0, tiles, top_end, 0)

        @pl.when(jnp.logical_and(p >= first_down, p < first_low))
        def _():
            @pl.when(part_of == 0)
            def _():
                acc[0:hidden, :] = jnp.zeros((hidden, dim), F32)

            lax.fori_loop(part_of * (tiles // 2), part_of * (tiles // 2) + tiles // 2, down_step, 0)

            @pl.when(part_of == 1)
            def _():
                for b in range(nz):
                    for c in range(2):
                        k = (b * 2 + c) * rows_d
                        td[0, b, c] = acc[k : k + rows_d, :].astype(BF)
                over_d(0).start()
                for c in later:
                    c.wait()

        @pl.when(jnp.logical_and(p >= first_low, p < end_low))
        def _():
            j = (p - first_low) // 2

            @pl.when(part_of == 0)
            def _():
                zero()

            with jax.named_scope("low"):
                lax.fori_loop(lo, lo + half, wide_step(j, False), 0)

            @pl.when(part_of == 1)
            def _():
                grads(nf + j)

        with jax.named_scope("events"):
            events(p)
        return 0

    lax.fori_loop(0, end_low + far + 1, phase, 0)
    results = [
        pltpu.make_async_copy(sum_gu, out_gu, in_sem.at[0]),
        pltpu.make_async_copy(sum_d, out_d, in_sem.at[1]),
    ]
    for c in results:
        c.start()

    all_ssq[me] = ssq[...]

    def scalar(k, slot):
        return pltpu.make_async_remote_copy(
            src_ref=ssq, dst_ref=all_ssq.at[slot], send_sem=q_send.at[k], recv_sem=q_recv.at[k],
            device_id={"dp": (me + k) % n}, device_id_type=MESH,
        )

    def tell(k, _):
        scalar(k, me).start()
        return 0

    lax.fori_loop(1, n, tell, 0)

    def told(k, _):
        scalar(k, (me + n - k) % n).wait()
        return 0

    with jax.named_scope("told"):
        lax.fori_loop(1, n, told, 0)
    for c in results:
        c.wait()
    total = jnp.sum(jnp.sum(jnp.sum(all_ssq[...], axis=0), axis=0, keepdims=True), axis=1, keepdims=True)
    count = 3 * 2 * dim * hidden
    factor[0, 0] = jnp.max(jnp.minimum(1.0, 0.5 * lax.rsqrt(total / count + 1e-30)))


def backward(n, h1, a1, dy, a0, hid, gu, dt):
    nz = n // 2
    tokens, dim = a0.shape
    hidden = dt.shape[2]
    nf, far = hidden // COLS, nz // 2
    rg, rd = dim // n, hidden // n
    anyspace = pl.BlockSpec(memory_space=pl.ANY)
    V = lambda *s: pltpu.VMEM(s, BF)
    W = lambda *s: pltpu.VMEM(s, F32)
    S = lambda *s: pltpu.SemaphoreType.DMA(s)
    return pl.pallas_call(
        functools.partial(backward_kernel, n),
        out_shape=[
            jax.ShapeDtypeStruct((2, 2, rg, hidden), BF),
            jax.ShapeDtypeStruct((2, rd, dim), BF),
            jax.ShapeDtypeStruct((1, 1), F32),
        ],
        in_specs=[anyspace] * 7,
        out_specs=[anyspace, anyspace, pl.BlockSpec(memory_space=pltpu.SMEM)],
        scratch_shapes=[
            V(tokens, dim),
            V(tokens, dim),
            V(tokens, dim),
            W(tokens, dim),
            V(2, dim, hidden),
            V(nf, 2 * COLS, dim),
            V(dim, hidden),
            V(3, TILE, hidden),
            V(2 * nf, 2, nz, 2, rg, COLS),
            V(2, nz, 2, rd, dim),
            V(2 * nf, 2, nz, rg, COLS),
            V(2, nz, rd, dim),
            V(2 * nf, 2, far, 2, rg, COLS),
            V(2, 2, far, rd, dim),
            V(2, 2, rg, hidden),
            V(2, rd, dim),
            W(dim, 2 * COLS),
            W(dim, COLS),
            W(8, 128),
            W(n, 8, 128),
            S(10),
            S(3),
            S(2 * nf + 2),
            S(2 * nf + 2),
            S(2 * nf, 2, far),
            S(2 * nf, 2, far),
            S(2, 2, far),
            S(2, 2, far),
            S(n),
            S(n),
        ],
        compiler_params=pltpu.CompilerParams(collective_id=1, has_side_effects=True, vmem_limit_bytes=61_000_000),
        cost_estimate=pl.CostEstimate(flops=28 * tokens * dim * hidden, bytes_accessed=40 << 20, transcendentals=0),
        name="backward",
    )(h1, a1, dy, a0, hid, gu, dt)


def adamw(w, m, v, g):
    m = 0.9 * m + 0.1 * g
    v = 0.95 * v + 0.05 * g * g
    step = m * lax.rsqrt(v + 1e-8) + 0.1 * w
    return (w - 0.02 * step).astype(BF), m, v


def solution(mesh):
    n = mesh.shape["dp"]

    def step(x, dy, *arrays):
        weights, m, v = (arrays[i : i + 3] for i in (0, 3, 6))
        h1, a1, hid, a0, gu, dt = forward(n, x[0], *weights)
        sum_gu, sum_d, factor = backward(n, h1, a1, dy[0], a0, hid, gu, dt)
        gradients = [sum_gu[:, 0].astype(F32), sum_gu[:, 1].astype(F32), sum_d.astype(F32)]
        factor = factor[0, 0]
        new = [adamw(w.astype(F32), m, v, g * factor) for w, m, v, g in zip(weights, m, v, gradients, strict=True)]
        return tuple(one[which] for which in range(3) for one in new)

    states, cut = P(("rep", "dp"), None, None), P(None, "dp", None)
    return jax.shard_map(
        step,
        mesh=mesh,
        in_specs=(states, states) + (cut,) * 9,
        out_specs=(P("rep", "dp", None),) * 9,
        check_vma=False,
    )
```

```python
import functools

import jax
import jax.numpy as jnp
from jax import lax
from jax.experimental import pallas as pl
from jax.experimental.pallas import tpu as pltpu
from jax.sharding import PartitionSpec as P

MESH = pl.DeviceIdType.MESH
BF, F32 = jnp.bfloat16, jnp.float32
VMEM_LIMIT = 66_500_000
TILE = 512
WIDE = 1024
COLS = 256


def dot(a, b):
    return jnp.dot(a, b, preferred_element_type=F32)


def dot_t(a, b):
    return lax.dot_general(a, b, (((0,), (0,)), ((), ())), preferred_element_type=F32)


def norm_scale(wide):
    return lax.rsqrt(jnp.mean(wide * wide, -1, keepdims=True) + 1e-6)


def places(n):
    nz = n // 2
    me = lax.axis_index("dp")
    z, core = me // 2, me % 2
    return me, z, core, ((z + 1) % nz) * 2 + core, ((z + nz - 1) % nz) * 2 + core, me + 1 - 2 * core


def barrier(devices):
    sem = pltpu.get_barrier_semaphore()
    for device in devices:
        pl.semaphore_signal(sem, inc=1, device_id={"dp": device}, device_id_type=MESH)
    pl.semaphore_wait(sem, len(devices))


def forward_kernel(n, x_hbm, wg_ref, wu_ref, wd_ref, h1_hbm, a1_hbm, hid_hbm, a0_hbm, gu_hbm, dt_hbm,
                   x, a0, hid, gu, d, dt, send_sem, recv_sem, in_sem, out_sem):
    nz = n // 2
    me, z, core, right, left, partner = places(n)
    tokens = x.shape[0]
    steps = tokens // TILE
    load = pltpu.make_async_copy(x_hbm, x, in_sem)
    load.start()
    barrier((right, left, partner))

    more, less = nz // 2, nz - 1 - nz // 2
    parts = [
        (wg_ref.at[0], gu, 0, more, less),
        (wu_ref.at[0], gu, 1, less, more),
        (wd_ref.at[0], d, 0, more, less),
        (wg_ref.at[1], gu, 2, less, more),
        (wu_ref.at[1], gu, 3, more, less),
        (wd_ref.at[1], d, 1, less, more),
    ]
    sent = []

    def block(i, chip, which):
        src, whole, first = parts[i][:3]
        rows = src.shape[0]
        return whole.at[first, pl.ds(pl.multiple_of((chip * 2 + which) * rows, 16), rows), :]

    def copy(i, k, src, dst, device):
        return pltpu.make_async_remote_copy(
            src_ref=src, dst_ref=dst, send_sem=send_sem.at[i, k], recv_sem=recv_sem.at[i, k],
            device_id={"dp": device}, device_id_type=MESH,
        )

    def send(i, k, src, dst, device):
        c = copy(i, k, src, dst, device)
        c.start()
        sent.append(c)

    def arrived(i, k, at):
        copy(i, k, at, at, partner).wait_recv()

    def begin(i):
        src, whole, first = parts[i][:3]
        rows = src.shape[0]
        own = block(i, z, core)
        send(i, 0, src, own, right)
        send(i, more, src, own, left)
        send(i, 2 * more, src, own, partner)
        whole[first, pl.ds(pl.multiple_of(me * rows, 16), rows), :] = src[...]

    def relay(i, s):
        hops_right, hops_left = parts[i][3:]
        if s <= hops_right:
            at = block(i, (z + nz - s) % nz, core)
            arrived(i, s - 1, at)
            if s < hops_right:
                send(i, s, at, at, right)
            send(i, 2 * more + s, at, at, partner)
        if s <= hops_left:
            at = block(i, (z + s) % nz, core)
            arrived(i, more + s - 1, at)
            if s < hops_left:
                send(i, more + s, at, at, left)
            send(i, 3 * more + s, at, at, partner)

    def finish(i):
        hops_right, hops_left = parts[i][3:]
        arrived(i, 2 * more, block(i, z, 1 - core))
        for s in range(1, hops_right + 1):
            arrived(i, 2 * more + s, block(i, (z + nz - s) % nz, 1 - core))
        for s in range(1, hops_left + 1):
            arrived(i, 3 * more + s, block(i, (z + s) % nz, 1 - core))

    outs = []

    def store(k, src, dst):
        c = pltpu.make_async_copy(src, dst, out_sem.at[k])
        c.start()
        outs.append(c)

    for i in range(3):
        begin(i)
    load.wait()

    def norm_step(t, _):
        at = pl.ds(pl.multiple_of(t * TILE, TILE), TILE)
        wide = x[at, :].astype(F32)
        a0[at, :] = (wide * norm_scale(wide)).astype(BF)
        return 0

    with jax.named_scope("gather0"):
        for s in range(1, more):
            if s < 3:
                lax.fori_loop((s - 1) * (steps // 2), s * (steps // 2), norm_step, 0)
            for i in range(3):
                relay(i, s)
        for i in range(3, 6):
            begin(i)
        relay(0, more)
        relay(1, more)
        finish(0)
        finish(1)
    store(0, a0, a0_hbm)

    def up_step(t, _):
        at = pl.ds(pl.multiple_of(t * TILE, TILE), TILE)
        a = a0[at, :]
        gate = dot(a, gu[0])
        up = dot(a, gu[1])
        hid[at, :] = (gate * jax.nn.sigmoid(gate) * up).astype(BF)
        return 0

    def down_step(t, _):
        at = pl.ds(pl.multiple_of(t * TILE, TILE), TILE)
        h = x[at, :] + dot(hid[at, :], d[0]).astype(BF)
        x[at, :] = h
        wide = h.astype(F32)
        a0[at, :] = (wide * norm_scale(wide)).astype(BF)
        return 0

    moves = [(2, 4), (3, 1), (4, 1), (5, 1), (3, 2), (4, 2), (5, 2), (3, 3), (4, 3), (5, 3), None, (3, 4), None, (4, 4), None, (5, 4)]
    each = steps // 8
    for q in range(8):
        with jax.named_scope("up"):
            lax.fori_loop(q * each, (q + 1) * each, up_step, 0)
        with jax.named_scope("move"):
            relay(*moves[q])
    store(1, hid, hid_hbm)
    store(2, gu.at[pl.ds(0, 2)], gu_hbm.at[pl.ds(0, 2)])
    outs[0].wait()
    finish(2)
    for q in range(8):
        with jax.named_scope("down"):
            lax.fori_loop(q * each, (q + 1) * each, down_step, 0)
        with jax.named_scope("move"):
            if moves[8 + q] is not None:
                relay(*moves[8 + q])
        at = pl.ds(q * each * TILE, each * TILE)
        store(6 + 2 * q, x.at[at, :], h1_hbm.at[at, :])
        store(7 + 2 * q, a0.at[at, :], a1_hbm.at[at, :])
        if q == 0:
            dt[0] = d[0].T
            store(3, dt.at[0], dt_hbm.at[0])
    with jax.named_scope("finish"):
        finish(3)
        finish(4)
    store(5, gu.at[pl.ds(2, 2)], gu_hbm.at[pl.ds(2, 2)])
    finish(5)
    dt[1] = d[1].T
    store(4, dt.at[1], dt_hbm.at[1])
    for c in sent:
        c.wait_send()
    for c in outs[1:]:
        c.wait()


def forward(n, x, wg, wu, wd):
    tokens, dim = x.shape
    hidden = wg.shape[2]
    anyspace, vmem = pl.BlockSpec(memory_space=pl.ANY), pl.BlockSpec(memory_space=pltpu.VMEM)
    shapes = [(tokens, dim), (tokens, dim), (tokens, hidden), (tokens, dim), (4, dim, hidden), (2, dim, hidden)]
    sems = 4 * (n // 4) + 1
    return pl.pallas_call(
        functools.partial(forward_kernel, n),
        out_shape=[jax.ShapeDtypeStruct(s, BF) for s in shapes],
        in_specs=[anyspace, vmem, vmem, vmem],
        out_specs=[anyspace] * 6,
        scratch_shapes=[
            pltpu.VMEM((tokens, dim), BF),
            pltpu.VMEM((tokens, dim), BF),
            pltpu.VMEM((tokens, hidden), BF),
            pltpu.VMEM((4, dim, hidden), BF),
            pltpu.VMEM((2, hidden, dim), BF),
            pltpu.VMEM((2, dim, hidden), BF),
            pltpu.SemaphoreType.DMA((6, sems)),
            pltpu.SemaphoreType.DMA((6, sems)),
            pltpu.SemaphoreType.DMA,
            pltpu.SemaphoreType.DMA((22,)),
        ],
        compiler_params=pltpu.CompilerParams(collective_id=0, has_side_effects=True, vmem_limit_bytes=VMEM_LIMIT),
        cost_estimate=pl.CostEstimate(flops=6 * tokens * dim * hidden, bytes_accessed=40 << 20, transcendentals=0),
        name="forward0",
    )(x, wg, wu, wd)


def backward_kernel(n, h1_hbm, a1_hbm, dy_hbm, a0_hbm, hid_hbm, gu_hbm, dt_hbm, out_gu, out_d, factor,
                    h1, a, dh, acc, gu, gt, dt, hid, tgu, td, pgu, pd, rgu, rd, sum_gu, sum_d, acc_gu, acc_d, ssq, all_ssq,
                    in_sem, hid_sem, p_send, p_recv, send_gu, recv_gu, send_d, recv_d, q_send, q_recv):
    nz = n // 2
    me, z, core, right, left, partner = places(n)
    tokens, dim = a.shape
    hidden = dt.shape[1]
    nf = hidden // COLS
    far, near = nz // 2, nz - 1 - nz // 2
    rows_g, rows_d = dim // n, hidden // n
    tiles, slots = tokens // TILE, hid.shape[0]
    half = tokens // WIDE // 2

    def load(k, src, dst):
        return pltpu.make_async_copy(src, dst, in_sem.at[k])

    def load_hid(t):
        slot = t % slots
        return pltpu.make_async_copy(hid_hbm.at[pl.ds(pl.multiple_of(t * TILE, TILE), TILE), :], hid.at[slot], hid_sem.at[slot])

    half_t = tokens // 2
    lo_t, hi_t = pl.ds(0, half_t), pl.ds(half_t, half_t)
    early = [
        load(0, gu_hbm.at[pl.ds(2, 2)], gu),
        load(1, dt_hbm.at[1], dt),
        load(2, a1_hbm.at[lo_t, :], a.at[lo_t, :]),
        load(3, dy_hbm.at[lo_t, :], dh.at[lo_t, :]),
    ]
    soon = [load(4, a1_hbm.at[hi_t, :], a.at[hi_t, :]), load(5, dy_hbm.at[hi_t, :], dh.at[hi_t, :])]
    whole_h1 = load(6, h1_hbm, h1)
    later = [load(7, a0_hbm, a), load(8, gu_hbm.at[pl.ds(0, 2)], gu), load(9, dt_hbm.at[0], dt)]
    for c in early:
        c.start()

    sem = pltpu.get_barrier_semaphore()
    for k in range(1, n):
        pl.semaphore_signal(sem, inc=1, device_id={"dp": (me + k) % n}, device_id_type=MESH)
    pl.semaphore_wait(sem, n - 1)

    ssq[...] = jnp.zeros_like(ssq)

    def begin_step(t, _):
        acc[pl.ds(pl.multiple_of(t * TILE, TILE), TILE), :] = jnp.zeros((TILE, dim), F32)
        return 0

    lax.fori_loop(0, tiles, begin_step, 0)
    early[0].wait()
    for j in range(nf):
        for i in range(2):
            gt[j, i * COLS : (i + 1) * COLS, :] = gu[i, :, j * COLS : (j + 1) * COLS].T
    for c in early[1:]:
        c.wait()
    for c in soon:
        c.start()

    def over_gu(q):
        return pltpu.make_async_remote_copy(
            src_ref=tgu.at[q, :, :, 1 - core], dst_ref=pgu.at[q], send_sem=p_send.at[q], recv_sem=p_recv.at[q],
            device_id={"dp": partner}, device_id_type=MESH,
        )

    def over_d(layer):
        k = 2 * nf + layer
        return pltpu.make_async_remote_copy(
            src_ref=td.at[layer, :, 1 - core], dst_ref=pd.at[layer], send_sem=p_send.at[k], recv_sem=p_recv.at[k],
            device_id={"dp": partner}, device_id_type=MESH,
        )

    def sides(odd):
        sign = 1 - 2 * odd

        def chip(way, s):
            return (z + 2 * nz + sign * (far - s)) % nz if way == 0 else (z + 2 * nz - sign * (near - s)) % nz

        def device(way):
            return ((z + nz + (sign if way == 0 else -sign)) % nz) * 2 + core

        return chip, device

    def squared(v):
        g = v.astype(F32)
        g = g * g
        while g.ndim > 2:
            g = jnp.sum(g, axis=0)
        g = jnp.sum(g, axis=0, keepdims=True)
        total = g[:, 0:128]
        for k in range(1, g.shape[1] // 128):
            total = total + g[:, k * 128 : (k + 1) * 128]
        ssq[0:1, :] += total

    class Gu:
        def __init__(self, q):
            self.q = q
            self.chip, self.device = sides(q % 2)

        def over(self):
            return over_gu(self.q)

        def term(self, b):
            return tgu[self.q, :, b, core].astype(F32) + pgu[self.q, :, b].astype(F32)

        def keep(self, b, v):
            tgu[self.q, :, b, core] = v

        def got(self, way, s):
            return rgu[self.q, way, s].astype(F32)

        def move(self, way, s):
            return pltpu.make_async_remote_copy(
                src_ref=tgu.at[self.q, :, self.chip(way, s), core], dst_ref=rgu.at[self.q, way, s],
                send_sem=send_gu.at[self.q, way, s], recv_sem=recv_gu.at[self.q, way, s],
                device_id={"dp": self.device(way)}, device_id_type=MESH,
            )

        def put(self, v):
            layer, j = 1 - self.q // nf, self.q % nf
            sum_gu[layer, :, :, pl.ds(pl.multiple_of(j * COLS, COLS), COLS)] = v

    class Down:
        def __init__(self, layer):
            self.layer = layer
            self.chip, self.device = sides(layer)

        def over(self):
            return over_d(self.layer)

        def term(self, b):
            return td[self.layer, b, core].astype(F32) + pd[self.layer, b].astype(F32)

        def keep(self, b, v):
            td[self.layer, b, core] = v

        def got(self, way, s):
            return rd[self.layer, way, s].astype(F32)

        def move(self, way, s):
            return pltpu.make_async_remote_copy(
                src_ref=td.at[self.layer, self.chip(way, s), core], dst_ref=rd.at[self.layer, way, s],
                send_sem=send_d.at[self.layer, way, s], recv_sem=recv_d.at[self.layer, way, s],
                device_id={"dp": self.device(way)}, device_id_type=MESH,
            )

        def put(self, v):
            sum_d[self.layer] = v

    def event(part, s):
        def on(way):
            b = part.chip(way, s)
            part.move(way, s - 1).wait()
            part.keep(b, (part.got(way, s - 1) + part.term(b)).astype(BF))
            part.move(way, s).start()

        @pl.when(s == 0)
        def _():
            part.over().wait()
            for way in range(2):
                b = part.chip(way, s)
                part.keep(b, part.term(b).astype(BF))
            for way in range(2):
                part.move(way, s).start()

        @pl.when(jnp.logical_and(s > 0, s < far))
        def _():
            on(0)

        @pl.when(jnp.logical_and(s > 0, s < near))
        def _():
            on(1)

        @pl.when(s == far)
        def _():
            part.move(0, far - 1).wait()
            part.move(1, near - 1).wait()
            v = (part.term(z) + part.got(0, far - 1) + part.got(1, near - 1)).astype(BF)
            part.put(v)
            squared(v)

    first_top, first_down, first_low = 0, 2 * nf, 2 * nf + 2
    end_low = first_low + 2 * nf

    def ready(q):
        return 2 * (q + q // nf)

    def events(p):
        def each_gu(k, _):
            q = (p + 1) // 2 - far // 2 - 2 + k
            s = p - (2 * q + 2)
            s = s - 2 * jnp.where(q >= nf, 1, 0)

            @pl.when(jnp.logical_and(jnp.logical_and(q >= 0, q < 2 * nf), jnp.logical_and(s >= 0, s <= far)))
            def _():
                event(Gu(q), s)

            return 0

        def each_d(k, _):
            s = p - (first_down + 2 * k)

            @pl.when(jnp.logical_and(s >= 0, s <= far))
            def _():
                event(Down(1 - k), s)

            return 0

        @pl.when(jnp.logical_and(p >= first_down, p < first_down + far + 3))
        def _():
            lax.fori_loop(0, 2, each_d, 0)

        lax.fori_loop(0, far // 2 + 2, each_gu, 0)

    def grads(q):
        for b in range(nz):
            for c in range(2):
                k = (b * 2 + c) * rows_g
                for i in range(2):
                    tgu[q, i, b, c] = acc_gu[k : k + rows_g, i * COLS : (i + 1) * COLS].astype(BF)
        over_gu(q).start()

    def wide_step(j, with_top):
        cols = pl.ds(pl.multiple_of(j * COLS, COLS), COLS)

        def body(t, _):
            at = pl.ds(pl.multiple_of(t * WIDE, WIDE), WIDE)
            rows = a[at, :]
            by_y = dh[at, :]
            gate = dot(rows, gu[0, :, cols])
            up = dot(rows, gu[1, :, cols])
            by_hid = dot(by_y, dt[:, cols]).astype(BF).astype(F32)
            sig = jax.nn.sigmoid(gate)
            act = gate * sig
            by_up = (by_hid * act).astype(BF)
            by_gate = (by_hid * up * (sig + act * (1.0 - sig))).astype(BF)
            by_both = jnp.concatenate([by_gate, by_up], axis=1)
            acc_gu[...] += dot_t(rows, by_both)
            if with_top:
                acc_d[...] += dot_t(by_y, (act * up).astype(BF))
                acc[at, :] += dot(by_both, gt[j])
            return 0

        return body

    def top_end(t, _):
        at = pl.ds(pl.multiple_of(t * TILE, TILE), TILE)
        wide = h1[at, :].astype(F32)
        scale = norm_scale(wide)
        by_a = acc[at, :].astype(BF).astype(F32)
        by_h = scale * by_a - wide * (scale * scale * scale * jnp.mean(by_a * wide, -1, keepdims=True))
        dh[at, :] = dh[at, :] + by_h.astype(BF)
        return 0

    def down_step(t, _):
        load_hid(t).wait()
        acc[0:hidden, :] += dot_t(hid[t % slots], dh[pl.ds(pl.multiple_of(t * TILE, TILE), TILE), :])

        @pl.when(t + slots < tiles)
        def _():
            load_hid(t + slots).start()

        return 0

    def zero():
        acc_gu[...] = jnp.zeros_like(acc_gu)

    def phase(p, _):
        part_of = p % 2
        lo = part_of * half

        @pl.when(p < first_down)
        def _():
            j = p // 2

            @pl.when(p == 1)
            def _():
                for c in soon:
                    c.wait()
                whole_h1.start()
                for t in range(slots):
                    load_hid(t).start()

            @pl.when(part_of == 0)
            def _():
                zero()
                acc_d[...] = jnp.zeros_like(acc_d)

            with jax.named_scope("top"):
                lax.fori_loop(lo, lo + half, wide_step(j, True), 0)

            @pl.when(part_of == 1)
            def _():
                grads(j)
                down = acc_d[...].T.astype(BF)
                for i in range(COLS // 16):
                    row = j * COLS + i * 16
                    device = row // rows_d
                    td[1, device // 2, device % 2, pl.ds(pl.multiple_of(row % rows_d, 16), 16), :] = down[i * 16 : i * 16 + 16, :]

            @pl.when(p == first_down - 1)
            def _():
                over_d(1).start()
                for c in later:
                    c.start()
                whole_h1.wait()
                with jax.named_scope("topend"):
                    lax.fori_loop(0, tiles, top_end, 0)

        @pl.when(jnp.logical_and(p >= first_down, p < first_low))
        def _():
            @pl.when(part_of == 0)
            def _():
                acc[0:hidden, :] = jnp.zeros((hidden, dim), F32)

            lax.fori_loop(part_of * (tiles // 2), part_of * (tiles // 2) + tiles // 2, down_step, 0)

            @pl.when(part_of == 1)
            def _():
                for b in range(nz):
                    for c in range(2):
                        k = (b * 2 + c) * rows_d
                        td[0, b, c] = acc[k : k + rows_d, :].astype(BF)
                over_d(0).start()
                for c in later:
                    c.wait()

        @pl.when(jnp.logical_and(p >= first_low, p < end_low))
        def _():
            j = (p - first_low) // 2

            @pl.when(part_of == 0)
            def _():
                zero()

            with jax.named_scope("low"):
                lax.fori_loop(lo, lo + half, wide_step(j, False), 0)

            @pl.when(part_of == 1)
            def _():
                grads(nf + j)

        with jax.named_scope("events"):
            events(p)
        return 0

    lax.fori_loop(0, end_low + far + 1, phase, 0)
    results = [
        pltpu.make_async_copy(sum_gu, out_gu, in_sem.at[0]),
        pltpu.make_async_copy(sum_d, out_d, in_sem.at[1]),
    ]
    for c in results:
        c.start()

    all_ssq[me] = ssq[...]

    def scalar(k, slot):
        return pltpu.make_async_remote_copy(
            src_ref=ssq, dst_ref=all_ssq.at[slot], send_sem=q_send.at[k], recv_sem=q_recv.at[k],
            device_id={"dp": (me + k) % n}, device_id_type=MESH,
        )

    def tell(k, _):
        scalar(k, me).start()
        return 0

    lax.fori_loop(1, n, tell, 0)

    def told(k, _):
        scalar(k, (me + n - k) % n).wait()
        return 0

    with jax.named_scope("told"):
        lax.fori_loop(1, n, told, 0)
    for c in results:
        c.wait()
    total = jnp.sum(jnp.sum(jnp.sum(all_ssq[...], axis=0), axis=0, keepdims=True), axis=1, keepdims=True)
    count = 3 * 2 * dim * hidden
    factor[0, 0] = jnp.max(jnp.minimum(1.0, 0.5 * lax.rsqrt(total / count + 1e-30)))


def backward(n, h1, a1, dy, a0, hid, gu, dt):
    nz = n // 2
    tokens, dim = a0.shape
    hidden = dt.shape[2]
    nf, far = hidden // COLS, nz // 2
    rg, rd = dim // n, hidden // n
    anyspace = pl.BlockSpec(memory_space=pl.ANY)
    V = lambda *s: pltpu.VMEM(s, BF)
    W = lambda *s: pltpu.VMEM(s, F32)
    S = lambda *s: pltpu.SemaphoreType.DMA(s)
    return pl.pallas_call(
        functools.partial(backward_kernel, n),
        out_shape=[
            jax.ShapeDtypeStruct((2, 2, rg, hidden), BF),
            jax.ShapeDtypeStruct((2, rd, dim), BF),
            jax.ShapeDtypeStruct((1, 1), F32),
        ],
        in_specs=[anyspace] * 7,
        out_specs=[anyspace, anyspace, pl.BlockSpec(memory_space=pltpu.SMEM)],
        scratch_shapes=[
            V(tokens, dim),
            V(tokens, dim),
            V(tokens, dim),
            W(tokens, dim),
            V(2, dim, hidden),
            V(nf, 2 * COLS, dim),
            V(dim, hidden),
            V(3, TILE, hidden),
            V(2 * nf, 2, nz, 2, rg, COLS),
            V(2, nz, 2, rd, dim),
            V(2 * nf, 2, nz, rg, COLS),
            V(2, nz, rd, dim),
            V(2 * nf, 2, far, 2, rg, COLS),
            V(2, 2, far, rd, dim),
            V(2, 2, rg, hidden),
            V(2, rd, dim),
            W(dim, 2 * COLS),
            W(dim, COLS),
            W(8, 128),
            W(n, 8, 128),
            S(10),
            S(3),
            S(2 * nf + 2),
            S(2 * nf + 2),
            S(2 * nf, 2, far),
            S(2 * nf, 2, far),
            S(2, 2, far),
            S(2, 2, far),
            S(n),
            S(n),
        ],
        compiler_params=pltpu.CompilerParams(collective_id=1, has_side_effects=True, vmem_limit_bytes=61_000_000),
        cost_estimate=pl.CostEstimate(flops=28 * tokens * dim * hidden, bytes_accessed=40 << 20, transcendentals=0),
        name="backward",
    )(h1, a1, dy, a0, hid, gu, dt)


def adamw(w, m, v, g):
    m = 0.9 * m + 0.1 * g
    v = 0.95 * v + 0.05 * g * g
    step = m * lax.rsqrt(v + 1e-8) + 0.1 * w
    return (w - 0.02 * step).astype(BF), m, v


def solution(mesh):
    n = mesh.shape["dp"]

    def step(x, dy, *arrays):
        weights, m, v = (arrays[i : i + 3] for i in (0, 3, 6))
        h1, a1, hid, a0, gu, dt = forward(n, x[0], *weights)
        sum_gu, sum_d, factor = backward(n, h1, a1, dy[0], a0, hid, gu, dt)
        gradients = [sum_gu[:, 0].astype(F32), sum_gu[:, 1].astype(F32), sum_d.astype(F32)]
        factor = factor[0, 0]
        new = [adamw(w.astype(F32), m, v, g * factor) for w, m, v, g in zip(weights, m, v, gradients, strict=True)]
        return tuple(one[which] for which in range(3) for one in new)

    states, cut = P(("rep", "dp"), None, None), P(None, "dp", None)
    return jax.shard_map(
        step,
        mesh=mesh,
        in_specs=(states, states) + (cut,) * 9,
        out_specs=(P("rep", "dp", None),) * 9,
        check_vma=False,
    )
```
